512 devices in a mesh: grid: 64 (over z, x, core), col: 8 (over y).
Axes of the slice: x: 4, y: 8, z: 8, core: 2. Of those that a mesh axis runs over, the one named last changes fastest.
Arguments:
- density: bfloat16 [16384, 16384], P('grid', 'col'), may hold values from -0.125 to 0.125
- centres: float32 [3, 16384], replicated, may hold values from -0.4 to 0.4
- exponents: float32 [16384], replicated, may hold values from 2 to 16
- coords: float32 [256, 3, 256], P('grid'), may hold values from -0.4 to 0.4
- weights: float32 [256, 256], P('grid'), may hold values from 0.078125 to 0.78125
- core_density: float32 [256, 256], P('grid'), may hold values from 0.3 to 3
- counts: int32 [256], P('grid'), may hold values from 1 to 256, 16384 in all
- blocks: int32 [256, 8], replicated, may hold values from 0 to 127, as said below
Outputs:
- potential_matrix_xc: float32 [16384, 16384], P('grid', 'col')
- orbital_charge_samples: float32 [256, 256], P('grid')
- xc_batch_amounts: float32 [256], P('grid')
The draws below stay inside these ranges and needn't reach their ends.
Inputs may be any that keep to these rules, and one draw needn't show every extreme that they name: Entry c of a batch's row names a block in the c-th of 8 equal runs of 16 blocks; for one grid index's 4 batches the values // 2 in one column c are distinct. The points in use are the first counts[b] slots.
All inputs are finite; a program needn't handle non-finite values. No bound on the sum of `counts` on one device may be relied on, other than what follows from the above.
Results may differ from the reference program's by a relative error of at most 0.0028.
Values may be sent and summed in bfloat16 or wider, within the bound.
No kernel may reach another device: no remote copies, remote signals or barrier semaphores. Data moves between devices by JAX's collectives and lax.ppermute only.
A program may use at most 64 MiB of HBM per device.

```python
import math
import jax
import jax.numpy as jnp
import numpy as np
from jax import lax

NBF = 16384
BLK = 128
NB = 4
PTS = 256
RB = 2
BATCHES = 256
N_GRID = 64
N_COL = 8


def draw_blocks(key, part):
    groups_per = N_GRID // N_COL
    scores = jax.random.randint(key, (N_GRID, N_COL, groups_per), 0, 1 << 20)
    scores = scores * groups_per + jnp.arange(groups_per, dtype=jnp.int32)[None, None, :]
    ranking = jnp.argsort(scores, axis=2)[:, :, :NB].astype(jnp.int32)
    inner_rows = jax.random.randint(jax.random.fold_in(key, 7), (N_GRID, N_COL, NB), 0, RB)
    owner_grid = jnp.arange(N_COL, dtype=jnp.int32)[None, :, None] * groups_per + ranking
    chosen = owner_grid * RB + inner_rows
    return jnp.transpose(chosen, (0, 2, 1)).reshape(N_GRID * NB, N_COL).astype(jnp.int32)


def block_scale(key, dims, shards, low, high):
    level = 1.0
    for dim, shards_of in shards:
        steps = jax.random.uniform(jax.random.fold_in(jax.random.fold_in(key, 6), dim), (shards_of,), jnp.float32, low / len(shards), high / len(shards))
        level = level * jnp.repeat(jnp.exp(steps), dims[dim] // shards_of).reshape((-1,) + (1,) * (len(dims) - 1 - dim))
    return level


def profile(count, total, most, lean):
    weights = [(1 << 20) // math.isqrt(standing ** lean) + 1 for standing in range(2, count + 1)]
    spare, holding = total - most - (count - 1), [1] * (count - 1)
    while spare > 0:
        free = [i for i in range(count - 1) if holding[i] < most]
        mass, left = sum([weights[i] for i in free]), spare
        for i in free:
            extra = min(most - holding[i], max(1, left * weights[i] // mass), spare)
            holding[i] = holding[i] + extra
            spare = spare - extra
    return np.array([most] + holding)


def ragged_sizes(rng, number_of, total, limit, slope):
    if number_of == 2:
        one = jax.random.randint(rng, (), max(1, total - limit), min(limit, total - 1) + 1)
        return jnp.stack([one, total - one])
    sizes = jnp.asarray(profile(number_of, total, limit, slope), jnp.int32)
    couples = (number_of - 1) // 2
    donor, taker = sizes[1:1 + 2 * couples:2], sizes[2:2 + 2 * couples:2]
    room = jnp.minimum(donor - 1, limit - taker)
    moved = jax.random.randint(jax.random.fold_in(rng, 1), (couples,), 0, 1 << 20) % (room + 1)
    sizes = sizes.at[1:1 + 2 * couples:2].set(donor - moved).at[2:2 + 2 * couples:2].set(taker + moved)
    return sizes[jax.random.permutation(jax.random.fold_in(rng, 2), number_of)]


def noise(own_key, extent, width, most, pieces=(), held_as=jnp.bfloat16):
    drawn = width * jax.random.normal(own_key, extent, jnp.float32)
    if pieces:
        drawn = drawn * block_scale(own_key, extent, pieces, -0.22, 0.18)
    return jnp.clip(drawn, -most, most).astype(held_as)


def setup_inputs(seed: int = 0) -> dict:
    key_list = jax.random.split(jax.random.key(seed), 9)
    density = noise(key_list[0], (NBF, NBF), (20.0 / (N_COL * BLK)), 0.125, ((0, 64), (1, 8)))
    centres = jnp.clip(jax.random.uniform(key_list[1], (3, NBF), jnp.float32, -0.4, 0.4), -0.4, 0.4)
    exponents = jnp.clip(jnp.exp(jax.random.uniform(key_list[2], (NBF,), jnp.float32, math.log(2.0), math.log(16.0))), 2.0, 16.0)
    coords = jnp.clip(jax.random.uniform(key_list[3], (BATCHES, 3, PTS), jnp.float32, -0.4, 0.4) * block_scale(key_list[3], (BATCHES, 3, PTS), ((0, 64),), -0.4, 0.0), -0.4, 0.4)
    weights = jnp.clip(jnp.exp(math.log(0.78125) - 2.3025851 * jax.random.uniform(key_list[4], (BATCHES, PTS), jnp.float32) ** block_scale(key_list[4], (BATCHES, PTS), ((0, 64),), -0.2, 0.2)), 0.078125, 0.78125)
    core_density = jnp.clip(jnp.exp(math.log(3.0) - 2.3025851 * jax.random.uniform(key_list[5], (BATCHES, PTS), jnp.float32) ** block_scale(key_list[5], (BATCHES, PTS), ((0, 64),), -0.2, 0.2)), 0.3, 3.0)
    counts = ragged_sizes(key_list[6], BATCHES, BATCHES * PTS // 4, PTS, 2).astype(jnp.int32)
    blocks = draw_blocks(jax.random.fold_in(key_list[8], 71), 0)
    return dict(density=density, centres=centres, exponents=exponents, coords=coords, weights=weights, core_density=core_density, counts=counts, blocks=blocks)


kappa_pbe = 0.804
mu_coef = 0.2195
slater = -0.7385587663820224
grad_scale = 4.0 * (3.0 * math.pi ** 2) ** (2.0 / 3.0)
soft_square = 0.25

def pbe_energy(total, grad_square):
    regular = 0.5 * (total + jnp.sqrt(total * total + soft_square))
    scaled = grad_scale * jnp.power(regular, 8.0 / 3.0)
    enhance = 1.0 + kappa_pbe - kappa_pbe * kappa_pbe * scaled / (kappa_pbe * scaled + mu_coef * grad_square)
    return slater * jnp.power(regular, 4.0 / 3.0) * enhance

def xc_kernel(total, grad_square):
    total_functional_sum, pullback = jax.vjp(pbe_energy, total, grad_square)
    charge_derivative, deriv_sigma = pullback(jnp.ones_like(total_functional_sum))
    return (total_functional_sum, charge_derivative, deriv_sigma)

def basis(points, centre_rows, rate_rows):
    offset = points[:, :, None] - centre_rows[:, None, :]
    distance = lax.optimization_barrier(jnp.sum(offset * offset, axis=0))
    value_entries = jnp.exp(-rate_rows[None, :] * distance)
    slopes = -2.0 * rate_rows[None, None, :] * offset * value_entries[None]
    return (value_entries, slopes)

def reference(density, centres, exponents, coords, weights, core_density, counts, blocks):
    offsets = jnp.arange(BLK, dtype=jnp.int32)
    point_ids = jnp.arange(PTS, dtype=jnp.int32)

    def one_batch(matrix, inputs):
        points, point_weights, core, count, block_row = inputs
        func_index = (block_row[:, None] * BLK + offsets[None, :]).reshape(-1).astype(jnp.int32)
        value_entries, slopes = basis(points, jnp.take(centres, func_index, axis=1), jnp.take(exponents, func_index))
        sub_matrix = jnp.take(jnp.take(density, func_index, axis=0), func_index, axis=1)
        phi_low = value_entries.astype(jnp.bfloat16)
        right_sum = jnp.dot(phi_low, sub_matrix, preferred_element_type=jnp.float32)
        left_sum = lax.dot_general(phi_low, sub_matrix, (((1,), (1,)), ((), ())), preferred_element_type=jnp.float32)
        live_mask = (point_ids < count).astype(jnp.float32)
        valence = live_mask * lax.optimization_barrier(jnp.sum(value_entries * right_sum, axis=1))
        gradient = live_mask[None, :] * (lax.optimization_barrier(jnp.sum(slopes * left_sum[None], axis=2)) + lax.optimization_barrier(jnp.sum(slopes * right_sum[None], axis=2)))
        grad_square = lax.optimization_barrier(jnp.sum(gradient * gradient, axis=0))
        total_functional_sum, charge_derivative, deriv_sigma = xc_kernel(valence + core, grad_square)
        point_scale = point_weights * live_mask
        fweight = point_scale * charge_derivative
        hweight = (2.0 * point_scale * deriv_sigma)[None, :] * gradient
        batch_energy = jnp.sum(point_scale * total_functional_sum)
        across = lax.optimization_barrier(jnp.sum(hweight[:, :, None] * slopes, axis=0))
        along = fweight[:, None] * value_entries + across
        left_side = jnp.concatenate([phi_low, across.astype(jnp.bfloat16)], axis=0)
        right_side = jnp.concatenate([along.astype(jnp.bfloat16), phi_low], axis=0)
        block_result_value = lax.dot_general(left_side, right_side, (((0,), (0,)), ((), ())), preferred_element_type=jnp.float32)
        matrix = matrix.at[func_index[:, None], func_index[None, :]].add(block_result_value)
        return (matrix, (valence, batch_energy))
    start = jnp.zeros((NBF, NBF), jnp.float32)
    matrix, (valence_all, energy_all) = lax.scan(one_batch, start, (coords, weights, core_density, counts, blocks))
    return (matrix, valence_all, energy_all)
```

```python
import jax
import jax.numpy as jnp
from jax import lax
from jax.experimental import pallas as pl
from jax.experimental.pallas import tpu as pltpu
from jax.sharding import PartitionSpec as P
import math

BLK = 128
NB = 4
LANES = 128
HALVES = 2

kappa_pbe = 0.804
mu_coef = 0.2195
slater = -0.7385587663820224
grad_scale = 4.0 * (3.0 * math.pi**2) ** (2.0 / 3.0)
soft_square = 0.25

SMEM = pl.BlockSpec(memory_space=pltpu.SMEM)
VMEM = pl.BlockSpec(memory_space=pltpu.VMEM)


def owner_of(table, column, batch):
    return lax.shift_right_logical(table[column, batch], 1)


def pack_kernel(place, table, counts, coords, out, tiles):
    first = place[0] * NB
    columns = table.shape[0]
    out[...] = jnp.zeros_like(out)
    for batch in range(NB):
        count = jnp.full((1, LANES), counts[batch].astype(jnp.float32), jnp.float32)
        for half in range(HALVES):
            for comp in range(3):
                tiles[batch, pl.ds(half * 4 + comp, 1), :] = coords[
                    comp, pl.ds(batch, 1), pl.ds(half * LANES, LANES)
                ]
            tiles[batch, pl.ds(half * 4 + 3, 1), :] = count
    for batch in range(NB):
        tile = tiles[batch]
        for column in range(columns):
            out[owner_of(table, column, first + batch)] = tile


def params_kernel(place, centres, exponents, rows_out, cols_out, tile):
    tile[...] = jnp.zeros_like(tile)

    def fill(block, out, slot):
        start = pl.multiple_of(block * BLK, BLK)
        tile[pl.ds(0, 3), :] = centres[:, pl.ds(start, BLK)]
        tile[pl.ds(3, 1), :] = exponents[pl.ds(block, 1), :]
        out[pl.ds(pl.multiple_of(slot * BLK, BLK), BLK), :] = tile[...].T

    row_blocks = rows_out.shape[0] // BLK
    col_blocks = cols_out.shape[0] // BLK
    for slot in range(row_blocks):
        fill(place[0] * row_blocks + slot, rows_out, slot)
    for slot in range(col_blocks):
        fill(place[1] * col_blocks + slot, cols_out, slot)


def offsets_of(params, point):
    return [point[comp] - params[:, comp : comp + 1] for comp in range(3)]


def values_of(params, offset):
    distance = offset[0] * offset[0] + offset[1] * offset[1] + offset[2] * offset[2]
    return jnp.exp(distance * (-params[:, 3:4]))


def total_rows(array):
    return jnp.sum(array, axis=0, keepdims=True)


def decode(entry):
    half = entry & 1
    block = lax.shift_right_logical(entry, 1) & 15
    row = lax.shift_right_logical(entry, 5) & 1
    source = lax.shift_right_logical(entry, 6)
    return source, row, block, half


def density_kernel(
    place, table, arrived, row_params, col_params, density, out, work, *, group
):
    rank = place[0]
    column = place[1]
    own = rank // group
    sources = arrived.shape[0]
    col_blocks = col_params.shape[0] // BLK
    out[...] = jnp.zeros_like(out)

    def list_source(source, filled):
        choice = jnp.int32(0)
        chosen = jnp.int32(0)
        found = jnp.int32(0)
        for batch in range(NB):
            block = table[own, source * NB + batch]
            match = lax.shift_right_logical(block, 1) == rank
            choice = jnp.where(match, source * NB + batch, choice)
            chosen = jnp.where(match, block, chosen)
            found = jnp.where(match, 1, found)
        target = table[column, choice] - column * col_blocks
        entry = source * 64 + (chosen & 1) * 32 + target * 2
        count = arrived[source, 3:4, :][0, 0]
        work[filled + 1] = entry
        filled = filled + found
        work[filled + 1] = entry + 1
        return filled + jnp.where(count > LANES, found, 0)

    filled = lax.fori_loop(0, sources, list_source, jnp.int32(0))
    work[0] = filled

    @pl.when((filled & 1) == 1)
    def _():
        work[filled + 1] = work[filled]

    def partial_sums(entry):
        source, row, block, half = decode(entry)
        point = [arrived[source, pl.ds(half * 4 + comp, 1), :] for comp in range(3)]
        row_start = pl.multiple_of(row * BLK, BLK)
        col_start = pl.multiple_of(block * BLK, BLK)
        rows = row_params[pl.ds(row_start, BLK), :]
        cols = col_params[pl.ds(col_start, BLK), :]
        tile = density[pl.ds(row_start, BLK), pl.ds(col_start, BLK)]
        row_offset = offsets_of(rows, point)
        row_values = values_of(rows, row_offset)
        col_offset = offsets_of(cols, point)
        col_values = values_of(cols, col_offset)
        right = lax.dot_general(
            tile,
            row_values.astype(jnp.bfloat16),
            (((0,), (0,)), ((), ())),
            preferred_element_type=jnp.float32,
        )
        left = lax.dot_general(
            tile,
            col_values.astype(jnp.bfloat16),
            (((1,), (0,)), ((), ())),
            preferred_element_type=jnp.float32,
        )
        col_product = col_values * right
        row_slope = (row_values * left) * (-2.0 * rows[:, 3:4])
        col_slope = col_product * (-2.0 * cols[:, 3:4])
        sums = [total_rows(col_product)]
        for comp in range(3):
            sums.append(total_rows(row_offset[comp] * row_slope + col_offset[comp] * col_slope))
        return source, half, sums

    def pair(step, carry):
        results = [partial_sums(work[2 * step + unit + 1]) for unit in range(2)]
        for source, half, sums in results:
            for comp in range(4):
                out[source, pl.ds(half * 4 + comp, 1), :] = sums[comp]
        return carry

    lax.fori_loop(0, (filled + 1) // 2, pair, 0)


def collect_kernel(place, table, arrived, out):
    first = place[0] * NB
    columns = table.shape[0]
    for batch in range(NB):
        total = arrived[owner_of(table, 0, first + batch)]
        for column in range(1, columns):
            total = total + arrived[owner_of(table, column, first + batch)]
        for copy in range(out.shape[0]):
            out[copy, batch] = total


def point_kernel(
    place, table, counts, partial, weights, core, out, charge_out, energy_out, summed, tiles, scale
):
    first = place[0] * NB
    columns = table.shape[0]
    for batch in range(NB):
        total = partial[0, batch]
        for column in range(1, partial.shape[0]):
            total = total + partial[column, batch]
        summed[pl.ds(batch * 8, 8), :] = total
    lane = lax.broadcasted_iota(jnp.int32, (1, LANES), 1)
    for batch in range(NB):
        for half in range(HALVES):
            place_row = pl.ds(batch * HALVES + half, 1)
            live = jnp.where(lane + half * LANES < counts[batch], 1.0, 0.0).astype(jnp.float32)
            scale[0, place_row, :] = live
            scale[1, place_row, :] = weights[pl.ds(batch, 1), pl.ds(half * LANES, LANES)]
            scale[2, place_row, :] = core[pl.ds(batch, 1), pl.ds(half * LANES, LANES)]
    live = scale[0]
    point_scale = scale[1] * live
    count_rows = NB * HALVES
    valence = live * summed[pl.ds(0, count_rows, stride=4), :]
    gradient = [live * summed[pl.ds(comp + 1, count_rows, stride=4), :] for comp in range(3)]
    grad_square = (
        gradient[0] * gradient[0] + gradient[1] * gradient[1] + gradient[2] * gradient[2]
    )
    total = valence + scale[2]
    root = jnp.sqrt(total * total + soft_square)
    regular = 0.5 * (total + root)
    third = jnp.exp(jnp.log(regular) * (1.0 / 3.0))
    four_thirds = regular * third
    scaled = grad_scale * four_thirds * four_thirds
    weighted = mu_coef * grad_square
    inverse = 1.0 / (kappa_pbe * scaled + weighted)
    fraction = scaled * inverse
    enhance = 1.0 + kappa_pbe - kappa_pbe * kappa_pbe * fraction
    energy = slater * four_thirds * enhance
    square = kappa_pbe * kappa_pbe * mu_coef
    deriv_sigma = slater * four_thirds * (square * fraction * inverse)
    enhance_slope = (
        -(kappa_pbe * kappa_pbe)
        * (weighted * inverse)
        * inverse
        * (grad_scale * (8.0 / 3.0) * four_thirds * third)
    )
    deriv_regular = slater * ((4.0 / 3.0) * third * enhance + four_thirds * enhance_slope)
    deriv_density = deriv_regular * (0.5 * (1.0 + total / root))
    fweight = point_scale * deriv_density
    factor = 2.0 * point_scale * deriv_sigma
    results = [fweight] + [factor * gradient[comp] for comp in range(3)]
    tiles[pl.ds(0, count_rows, stride=4), :] = results[0]
    for comp in range(3):
        tiles[pl.ds(comp + 1, count_rows, stride=4), :] = results[comp + 1]
    out[...] = jnp.zeros_like(out)
    for batch in range(NB):
        tile = tiles[pl.ds(batch * 8, 8), :]
        for column in range(columns):
            out[owner_of(table, column, first + batch)] = tile
    scale[0] = valence
    scale[1] = point_scale * energy
    for batch in range(NB):
        for half in range(HALVES):
            charge_out[pl.ds(batch, 1), pl.ds(half * LANES, LANES)] = scale[
                0, pl.ds(batch * HALVES + half, 1), :
            ]
        energy_out[batch] = jnp.sum(scale[1, pl.ds(batch * HALVES, HALVES), :])


def potential_kernel(work, arrived, factors, row_params, col_params, out):
    out[...] = jnp.zeros_like(out)
    filled = work[0]

    def tile_of(entry, keep):
        source, row, block, half = decode(entry)
        point = [arrived[source, pl.ds(half * 4 + comp, 1), :] for comp in range(3)]
        factor = [factors[source, pl.ds(half * 4 + comp, 1), :] * keep for comp in range(4)]
        row_start = pl.multiple_of(row * BLK, BLK)
        col_start = pl.multiple_of(block * BLK, BLK)

        def sides(params):
            offset = offsets_of(params, point)
            values = values_of(params, offset)
            along = (
                factor[1] * offset[0] + factor[2] * offset[1] + factor[3] * offset[2]
            ) * (-2.0 * params[:, 3:4])
            return values, along * values

        row_values, row_across = sides(row_params[pl.ds(row_start, BLK), :])
        col_values, col_across = sides(col_params[pl.ds(col_start, BLK), :])
        along = factor[0] * col_values + col_across
        left_side = jnp.concatenate(
            [row_values.astype(jnp.bfloat16), row_across.astype(jnp.bfloat16)], axis=1
        )
        right_side = jnp.concatenate(
            [along.astype(jnp.bfloat16), col_values.astype(jnp.bfloat16)], axis=1
        )
        product = lax.dot_general(
            left_side,
            right_side,
            (((1,), (1,)), ((), ())),
            preferred_element_type=jnp.float32,
        )
        return row_start, col_start, product

    def pair(step, carry):
        results = []
        for unit in range(2):
            index = 2 * step + unit
            keep = jnp.where(index < filled, 1.0, 0.0).astype(jnp.float32)
            results.append(tile_of(work[index + 1], keep))
        for row_start, col_start, product in results:
            place = (pl.ds(row_start, BLK), pl.ds(col_start, BLK))
            out[place] = out[place] + product
        return carry

    lax.fori_loop(0, (filled + 1) // 2, pair, 0)


def local(density, centres, exponents, coords, weights, core_density, counts, blocks):
    sources = lax.axis_size("grid")
    columns = lax.axis_size("col")
    rows, cols = density.shape
    points = coords.shape[2]
    f32 = jnp.float32
    params = pltpu.CompilerParams(vmem_limit_bytes=48 * 1024 * 1024)
    place = jnp.stack([lax.axis_index("grid"), lax.axis_index("col")]).astype(jnp.int32)
    table = blocks.T
    slots = jax.ShapeDtypeStruct((sources, 8, LANES), f32)

    outgoing = pl.pallas_call(
        pack_kernel,
        out_shape=slots,
        in_specs=[SMEM, SMEM, SMEM, VMEM],
        out_specs=VMEM,
        scratch_shapes=[pltpu.VMEM((NB, 8, LANES), f32)],
        compiler_params=params,
        name="pack",
    )(place, table, counts, coords.transpose(1, 0, 2))
    arrived = lax.all_to_all(outgoing, "grid", split_axis=0, concat_axis=0, tiled=True)
    row_params, col_params = pl.pallas_call(
        params_kernel,
        out_shape=(jax.ShapeDtypeStruct((rows, 8), f32), jax.ShapeDtypeStruct((cols, 8), f32)),
        in_specs=[SMEM, VMEM, VMEM],
        out_specs=(VMEM, VMEM),
        scratch_shapes=[pltpu.VMEM((8, LANES), f32)],
        compiler_params=params,
        name="params",
    )(place, centres, exponents.reshape(-1, LANES))
    partial, work = pl.pallas_call(
        lambda *refs: density_kernel(*refs, group=sources // columns),
        out_shape=(slots, jax.ShapeDtypeStruct((2 * sources + 8,), jnp.int32)),
        in_specs=[SMEM, SMEM, VMEM, VMEM, VMEM, VMEM],
        out_specs=(VMEM, SMEM),
        compiler_params=params,
        name="density",
    )(place, table, arrived, row_params, col_params, density)
    returned = lax.all_to_all(partial, "grid", split_axis=0, concat_axis=0, tiled=True)
    copies = pl.pallas_call(
        collect_kernel,
        out_shape=jax.ShapeDtypeStruct((columns, NB, 8, LANES), f32),
        in_specs=[SMEM, SMEM, VMEM],
        out_specs=VMEM,
        compiler_params=params,
        name="collect",
    )(place, table, returned)
    everything = lax.all_to_all(copies, "col", split_axis=0, concat_axis=0, tiled=True)
    sending, orbital_charge_samples, xc_batch_amounts = pl.pallas_call(
        point_kernel,
        out_shape=(
            slots,
            jax.ShapeDtypeStruct((NB, points), f32),
            jax.ShapeDtypeStruct((NB,), f32),
        ),
        in_specs=[SMEM, SMEM, SMEM, VMEM, VMEM, VMEM],
        out_specs=(VMEM, VMEM, SMEM),
        scratch_shapes=[
            pltpu.VMEM((NB * 8, LANES), f32),
            pltpu.VMEM((NB * 8, LANES), f32),
            pltpu.VMEM((3, 8, LANES), f32),
        ],
        compiler_params=params,
        name="points",
    )(place, table, counts, everything, weights, core_density)
    factors = lax.all_to_all(sending, "grid", split_axis=0, concat_axis=0, tiled=True)
    potential_matrix_xc = pl.pallas_call(
        potential_kernel,
        out_shape=jax.ShapeDtypeStruct((rows, cols), f32),
        in_specs=[SMEM, VMEM, VMEM, VMEM, VMEM],
        out_specs=VMEM,
        compiler_params=params,
        name="potential",
    )(work, arrived, factors, row_params, col_params)
    return (potential_matrix_xc, orbital_charge_samples, xc_batch_amounts)


def solution(mesh):
    return jax.shard_map(
        local,
        mesh=mesh,
        in_specs=(
            P("grid", "col"),
            P(),
            P(),
            P("grid", None, None),
            P("grid", None),
            P("grid", None),
            P("grid"),
            P(),
        ),
        out_specs=(P("grid", "col"), P("grid", None), P("grid")),
        check_vma=False,
    )
```

```python
from functools import partial
import math

import jax
import jax.numpy as jnp
from jax import lax
from jax.experimental import pallas as pl
from jax.experimental.pallas import tpu as pltpu
from jax.sharding import PartitionSpec as P

BLK = 128
NB = 4
LANES = 128
HALVES = 2

kappa_pbe = 0.804
mu_coef = 0.2195
slater = -0.7385587663820224
grad_scale = 4.0 * (3.0 * math.pi**2) ** (2.0 / 3.0)
soft_square = 0.25

SMEM = pl.BlockSpec(memory_space=pltpu.SMEM)
VMEM = pl.BlockSpec(memory_space=pltpu.VMEM)


LOG2E = math.log2(math.e)
SLOPE = 2.0 * math.log(2.0)
HBM = pl.BlockSpec(memory_space=pltpu.HBM)


def pack_kernel(table_hbm, counts_hbm, coords_hbm, out, slots, table, counts, coords, tiles, sems):
    copies = [
        pltpu.make_async_copy(source, target, sems.at[index])
        for index, (source, target) in enumerate(
            [(table_hbm, table), (counts_hbm, counts), (coords_hbm, coords)]
        )
    ]
    for copy in copies:
        copy.start()
    first = lax.axis_index("grid") * NB
    columns = table.shape[0]
    out[...] = jnp.zeros_like(out)
    for copy in copies:
        copy.wait()
    for batch in range(NB):
        count = jnp.full((1, LANES), counts[batch].astype(jnp.float32), jnp.float32)
        for half in range(HALVES):
            for comp in range(3):
                tiles[batch, pl.ds(half * 4 + comp, 1), :] = coords[
                    comp, pl.ds(batch, 1), pl.ds(half * LANES, LANES)
                ]
            tiles[batch, pl.ds(half * 4 + 3, 1), :] = count
    for batch in range(NB):
        tile = tiles[batch]
        for column in range(columns):
            slot = lax.shift_right_logical(table[column, first + batch], 1)
            slots[column * NB + batch] = slot
            out[slot] = tile


def prepare_kernel(table, centres, exponents, density, at_x, at_y, at_z, rate, forward, backward, work, tile, *, group):
    rank = lax.axis_index("grid")
    column = lax.axis_index("col")
    own = rank // group
    row_blocks = density.shape[0] // BLK
    col_blocks = density.shape[1] // BLK
    sources = table.shape[1] // NB
    basis = (at_x, at_y, at_z, rate)
    tile[...] = jnp.zeros_like(tile)

    def fill(block, slot):
        start = pl.multiple_of(block * BLK, BLK)
        tile[pl.ds(0, 3), :] = centres[:, pl.ds(start, BLK)]
        tile[pl.ds(3, 1), :] = exponents[pl.ds(block, 1), :] * (-LOG2E)
        upright = tile[...].T
        for comp in range(4):
            basis[comp][slot] = jnp.broadcast_to(upright[:, comp : comp + 1], (BLK, LANES))

    for slot in range(row_blocks):
        fill(rank * row_blocks + slot, slot)

    def fill_column(slot, carry):
        fill(column * col_blocks + slot, row_blocks + slot)
        start = pl.multiple_of(slot * BLK, BLK)
        for row in range(row_blocks):
            piece = density[pl.ds(row * BLK, BLK), pl.ds(start, BLK)]
            forward[slot, row] = piece
            backward[slot, row] = piece.T
        return carry

    lax.fori_loop(0, col_blocks, fill_column, 0)

    def list_sources(step, filled):
        for unit in range(4):
            source = step * 4 + unit
            code = jnp.int32(0)
            for batch in range(NB):
                part = table[own, source * NB + batch] ^ (2 * rank)
                code = jnp.where(part < 2, 8 + 2 * batch + part, code)
            choice = lax.shift_right_logical(code, 1) & 3
            target = table[column, source * NB + choice] - column * col_blocks
            work[filled + 1] = source * 64 + (code & 1) * 32 + target * 2
            filled = filled + lax.shift_right_logical(code, 3)
        return filled

    filled = lax.fori_loop(0, sources // 4, list_sources, jnp.int32(0))
    work[0] = filled
    work[filled + 1] = work[jnp.maximum(filled, 1)]


def total_rows(array):
    return jnp.sum(array, axis=0, keepdims=True)


def decode(entry):
    half = entry & 1
    block = lax.shift_right_logical(entry, 1) & 15
    row = lax.shift_right_logical(entry, 5) & 1
    source = lax.shift_right_logical(entry, 6)
    return source, row, block, half


def values_of(side, point):
    offset = [point[comp] - side(comp) for comp in range(3)]
    distance = offset[0] * offset[0] + offset[1] * offset[1] + offset[2] * offset[2]
    return jnp.exp2(distance * side(3))


def over_pairs(work, handle, carry):
    filled = work[0]

    def pair(step, carry):
        entries = [(work[2 * step + unit + 1], 2 * step + unit < filled) for unit in range(2)]
        return handle(entries, carry)

    return lax.fori_loop(0, lax.shift_right_logical(filled + 1, 1), pair, carry)


def density_kernel(work, arrived, at_x, at_y, at_z, rate, forward, backward, out, later):
    basis = (at_x, at_y, at_z, rate)
    row_blocks = forward.shape[1]
    out[...] = jnp.zeros_like(out)

    def partial_sums(entry):
        source, row, block, half = decode(entry)
        point = [arrived[source, pl.ds(half * 4 + comp, 1), :] for comp in range(3)]

        def row_side(comp):
            return basis[comp][row]

        def col_side(comp):
            return basis[comp][row_blocks + block]

        row_values = values_of(row_side, point)
        col_values = values_of(col_side, point)
        right = jnp.dot(
            backward[block, row], row_values.astype(jnp.bfloat16), preferred_element_type=jnp.float32
        )
        left = jnp.dot(
            forward[block, row], col_values.astype(jnp.bfloat16), preferred_element_type=jnp.float32
        )
        col_product = col_values * right
        col_slope = col_product * col_side(3)
        row_slope = row_values * left * row_side(3)
        slope = total_rows(row_slope + col_slope)
        sums = [total_rows(col_product)]
        for comp in range(3):
            moment = total_rows(row_slope * row_side(comp) + col_slope * col_side(comp))
            sums.append(SLOPE * (point[comp] * slope - moment))
        return source, half, sums

    def first_halves(entries, filled):
        for entry, real in entries:
            count = arrived[lax.shift_right_logical(entry, 6), 3:4, :][0, 0]
            later[filled + 1] = entry + 1
            filled = filled + jnp.where(jnp.logical_and(count > LANES, real), 1, 0)
        return halves(entries, filled)

    def halves(entries, carry):
        results = [partial_sums(entry) for entry, _ in entries]
        for source, half, sums in results:
            for comp in range(4):
                out[source, pl.ds(half * 4 + comp, 1), :] = sums[comp]
        return carry

    filled = over_pairs(work, first_halves, jnp.int32(0))
    later[0] = filled
    later[filled + 1] = later[jnp.maximum(filled, 1)]
    over_pairs(later, halves, 0)


def collect_kernel(slots, arrived, out):
    columns = slots.shape[0] // NB
    for batch in range(NB):
        total = arrived[slots[batch]]
        for column in range(1, columns):
            total = total + arrived[slots[column * NB + batch]]
        for copy in range(out.shape[0]):
            out[copy, batch] = total


def point_kernel(
    slots, counts, sums, weights, core, out, charge_out, energy_out, summed, tiles, scale
):
    columns = slots.shape[0] // NB
    for batch in range(NB):
        total = sums[0, batch]
        for column in range(1, sums.shape[0]):
            total = total + sums[column, batch]
        summed[pl.ds(batch * 8, 8), :] = total
    lane = lax.broadcasted_iota(jnp.int32, (1, LANES), 1)
    for batch in range(NB):
        for half in range(HALVES):
            place_row = pl.ds(batch * HALVES + half, 1)
            live = jnp.where(lane + half * LANES < counts[batch], 1.0, 0.0).astype(jnp.float32)
            scale[0, place_row, :] = live
            scale[1, place_row, :] = weights[pl.ds(batch, 1), pl.ds(half * LANES, LANES)]
            scale[2, place_row, :] = core[pl.ds(batch, 1), pl.ds(half * LANES, LANES)]
    live = scale[0]
    point_scale = scale[1] * live
    count_rows = NB * HALVES
    valence = live * summed[pl.ds(0, count_rows, stride=4), :]
    gradient = [live * summed[pl.ds(comp + 1, count_rows, stride=4), :] for comp in range(3)]
    grad_square = (
        gradient[0] * gradient[0] + gradient[1] * gradient[1] + gradient[2] * gradient[2]
    )
    total = valence + scale[2]
    root = jnp.sqrt(total * total + soft_square)
    regular = 0.5 * (total + root)
    third = jnp.exp(jnp.log(regular) * (1.0 / 3.0))
    four_thirds = regular * third
    scaled = grad_scale * four_thirds * four_thirds
    weighted = mu_coef * grad_square
    inverse = 1.0 / (kappa_pbe * scaled + weighted)
    fraction = scaled * inverse
    enhance = 1.0 + kappa_pbe - kappa_pbe * kappa_pbe * fraction
    energy = slater * four_thirds * enhance
    square = kappa_pbe * kappa_pbe * mu_coef
    deriv_sigma = slater * four_thirds * (square * fraction * inverse)
    enhance_slope = (
        -(kappa_pbe * kappa_pbe)
        * (weighted * inverse)
        * inverse
        * (grad_scale * (8.0 / 3.0) * four_thirds * third)
    )
    deriv_regular = slater * ((4.0 / 3.0) * third * enhance + four_thirds * enhance_slope)
    deriv_density = deriv_regular * (0.5 * (1.0 + total / root))
    fweight = point_scale * deriv_density
    factor = 2.0 * point_scale * deriv_sigma
    results = [fweight] + [factor * gradient[comp] for comp in range(3)]
    tiles[pl.ds(0, count_rows, stride=4), :] = results[0]
    for comp in range(3):
        tiles[pl.ds(comp + 1, count_rows, stride=4), :] = results[comp + 1]
    out[...] = jnp.zeros_like(out)
    for batch in range(NB):
        tile = tiles[pl.ds(batch * 8, 8), :]
        for column in range(columns):
            out[slots[column * NB + batch]] = tile
    scale[0] = valence
    scale[1] = point_scale * energy
    for batch in range(NB):
        for half in range(HALVES):
            charge_out[pl.ds(batch, 1), pl.ds(half * LANES, LANES)] = scale[
                0, pl.ds(batch * HALVES + half, 1), :
            ]
        energy_out[batch] = jnp.sum(scale[1, pl.ds(batch * HALVES, HALVES), :])


def potential_kernel(work, later, arrived, factors, at_x, at_y, at_z, rate, out):
    basis = (at_x, at_y, at_z, rate)
    row_blocks = out.shape[0] // BLK
    out[...] = jnp.zeros_like(out)

    def tile_of(entry, real):
        source, row, block, half = decode(entry)
        keep = jnp.where(real, 1.0, 0.0).astype(jnp.float32)
        point = [arrived[source, pl.ds(half * 4 + comp, 1), :] for comp in range(3)]
        factor = [factors[source, pl.ds(half * 4 + comp, 1), :] * keep for comp in range(4)]
        push = [SLOPE * factor[comp + 1] for comp in range(3)]
        along_point = push[0] * point[0] + push[1] * point[1] + push[2] * point[2]

        def turn(side):
            along_centre = push[0] * side(0) + push[1] * side(1) + push[2] * side(2)
            return (along_point - along_centre) * side(3)

        def row_side(comp):
            return basis[comp][row]

        def col_side(comp):
            return basis[comp][row_blocks + block]

        row_values = values_of(row_side, point)
        col_values = values_of(col_side, point)
        row_across = row_values * turn(row_side)
        along = col_values * (factor[0] + turn(col_side))
        left_side = jnp.concatenate(
            [row_values.astype(jnp.bfloat16), row_across.astype(jnp.bfloat16)], axis=1
        )
        right_side = jnp.concatenate(
            [along.astype(jnp.bfloat16), col_values.astype(jnp.bfloat16)], axis=1
        )
        product = lax.dot_general(
            left_side,
            right_side,
            (((1,), (1,)), ((), ())),
            preferred_element_type=jnp.float32,
        )
        row_start = pl.multiple_of(row * BLK, BLK)
        col_start = pl.multiple_of(block * BLK, BLK)
        return row_start, col_start, product

    def handle(entries, carry):
        results = [tile_of(entry, real) for entry, real in entries]
        for row_start, col_start, product in results:
            place = (pl.ds(row_start, BLK), pl.ds(col_start, BLK))
            out[place] = out[place] + product
        return carry

    over_pairs(work, handle, 0)
    over_pairs(later, handle, 0)


def local(density, centres, exponents, coords, weights, core_density, counts, blocks):
    sources = lax.axis_size("grid")
    columns = lax.axis_size("col")
    rows, cols = density.shape
    points = coords.shape[2]
    f32 = jnp.float32
    params = pltpu.CompilerParams(vmem_limit_bytes=16 * 1024 * 1024)
    table = blocks.T
    shape = jax.ShapeDtypeStruct
    messages = shape((sources, 8, LANES), f32)
    blocks_held = rows // BLK + cols // BLK
    tile_shape = shape((cols // BLK, rows // BLK, BLK, BLK), jnp.bfloat16)
    spread = shape((blocks_held, BLK, LANES), f32)
    listed = shape((sources + 8,), jnp.int32)

    outgoing, slots = pl.pallas_call(
        pack_kernel,
        out_shape=(messages, shape((columns * NB,), jnp.int32)),
        in_specs=[HBM, HBM, HBM],
        out_specs=(VMEM, SMEM),
        scratch_shapes=[
            pltpu.SMEM(table.shape, jnp.int32),
            pltpu.SMEM(counts.shape, jnp.int32),
            pltpu.VMEM((3, NB, points), f32),
            pltpu.VMEM((NB, 8, LANES), f32),
            pltpu.SemaphoreType.DMA((3,)),
        ],
        compiler_params=params,
        name="pack",
    )(
        *[
            pltpu.with_memory_space_constraint(array, pltpu.HBM)
            for array in (table, counts, coords.transpose(1, 0, 2))
        ]
    )
    arrived = lax.all_to_all(outgoing, "grid", split_axis=0, concat_axis=0, tiled=True)
    *basis, forward, backward, work = pl.pallas_call(
        partial(prepare_kernel, group=sources // columns),
        out_shape=(spread,) * 4 + (tile_shape, tile_shape, listed),
        in_specs=[SMEM, VMEM, VMEM, VMEM],
        out_specs=(VMEM,) * 6 + (SMEM,),
        scratch_shapes=[pltpu.VMEM((8, LANES), f32)],
        compiler_params=params,
        name="prepare",
    )(table, centres, exponents.reshape(-1, LANES), density)
    partials, later = pl.pallas_call(
        density_kernel,
        out_shape=(messages, listed),
        in_specs=[SMEM] + [VMEM] * 7,
        out_specs=(VMEM, SMEM),
        compiler_params=params,
        name="density",
    )(work, arrived, *basis, forward, backward)
    returned = lax.all_to_all(partials, "grid", split_axis=0, concat_axis=0, tiled=True)
    copies = pl.pallas_call(
        collect_kernel,
        out_shape=shape((columns, NB, 8, LANES), f32),
        in_specs=[SMEM, VMEM],
        out_specs=VMEM,
        compiler_params=params,
        name="collect",
    )(slots, returned)
    everything = lax.all_to_all(copies, "col", split_axis=0, concat_axis=0, tiled=True)
    sending, orbital_charge_samples, xc_batch_amounts = pl.pallas_call(
        point_kernel,
        out_shape=(messages, shape((NB, points), f32), shape((NB,), f32)),
        in_specs=[SMEM, SMEM, VMEM, VMEM, VMEM],
        out_specs=(VMEM, VMEM, SMEM),
        scratch_shapes=[
            pltpu.VMEM((NB * 8, LANES), f32),
            pltpu.VMEM((NB * 8, LANES), f32),
            pltpu.VMEM((3, 8, LANES), f32),
        ],
        compiler_params=params,
        name="points",
    )(slots, counts, everything, weights, core_density)
    factors = lax.all_to_all(sending, "grid", split_axis=0, concat_axis=0, tiled=True)
    potential_matrix_xc = pl.pallas_call(
        potential_kernel,
        out_shape=shape((rows, cols), f32),
        in_specs=[SMEM, SMEM] + [VMEM] * 6,
        out_specs=VMEM,
        compiler_params=params,
        name="potential",
    )(work, later, arrived, factors, *basis)
    return (potential_matrix_xc, orbital_charge_samples, xc_batch_amounts)


def solution(mesh):
    return jax.shard_map(
        local,
        mesh=mesh,
        in_specs=(
            P("grid", "col"),
            P(),
            P(),
            P("grid", None, None),
            P("grid", None),
            P("grid", None),
            P("grid"),
            P(),
        ),
        out_specs=(P("grid", "col"), P("grid", None), P("grid")),
        check_vma=False,
    )
```

```python
from functools import partial
import math

import jax
import jax.numpy as jnp
from jax import lax
from jax.experimental import pallas as pl
from jax.experimental.pallas import tpu as pltpu
from jax.sharding import PartitionSpec as P

BLK = 128
NB = 4
LANES = 128
HALVES = 2

kappa_pbe = 0.804
mu_coef = 0.2195
slater = -0.7385587663820224
grad_scale = 4.0 * (3.0 * math.pi**2) ** (2.0 / 3.0)
soft_square = 0.25

SMEM = pl.BlockSpec(memory_space=pltpu.SMEM)
VMEM = pl.BlockSpec(memory_space=pltpu.VMEM)


LOG2E = math.log2(math.e)
SLOPE = 2.0 * math.log(2.0)
HBM = pl.BlockSpec(memory_space=pltpu.HBM)


def pack_kernel(table_hbm, counts_hbm, coords_hbm, out, slots, table, counts, coords, tiles, sems):
    copies = [
        pltpu.make_async_copy(source, target, sems.at[index])
        for index, (source, target) in enumerate(
            [(table_hbm, table), (counts_hbm, counts), (coords_hbm, coords)]
        )
    ]
    for copy in copies:
        copy.start()
    first = lax.axis_index("grid") * NB
    columns = table.shape[0]
    out[...] = jnp.zeros_like(out)
    for copy in copies:
        copy.wait()
    for batch in range(NB):
        count = jnp.full((1, LANES), counts[batch].astype(jnp.float32), jnp.float32)
        for half in range(HALVES):
            for comp in range(3):
                tiles[batch, pl.ds(half * 4 + comp, 1), :] = coords[
                    comp, pl.ds(batch, 1), pl.ds(half * LANES, LANES)
                ]
            tiles[batch, pl.ds(half * 4 + 3, 1), :] = count
    for batch in range(NB):
        tile = tiles[batch]
        for column in range(columns):
            slot = lax.shift_right_logical(table[column, first + batch], 1)
            slots[column * NB + batch] = slot
            out[slot] = tile


def prepare_kernel(table, centres, exponents, density, row_params, col_params, forward, backward, work, tile, *, group):
    rank = lax.axis_index("grid")
    column = lax.axis_index("col")
    own = rank // group
    row_blocks = density.shape[0] // BLK
    col_blocks = density.shape[1] // BLK
    sources = table.shape[1] // NB
    tile[...] = jnp.zeros_like(tile)

    def fill(block, params, slot):
        start = pl.multiple_of(block * BLK, BLK)
        tile[pl.ds(0, 3), :] = centres[:, pl.ds(start, BLK)]
        tile[pl.ds(3, 1), :] = exponents[pl.ds(block, 1), :] * (-LOG2E)
        params[pl.ds(pl.multiple_of(slot * BLK, BLK), BLK), :] = tile[...].T

    for slot in range(row_blocks):
        fill(rank * row_blocks + slot, row_params, slot)

    def fill_column(slot, carry):
        fill(column * col_blocks + slot, col_params, slot)
        start = pl.multiple_of(slot * BLK, BLK)
        for row in range(row_blocks):
            piece = density[pl.ds(row * BLK, BLK), pl.ds(start, BLK)]
            forward[slot, row] = piece
            backward[slot, row] = piece.T
        return carry

    lax.fori_loop(0, col_blocks, fill_column, 0)

    def list_sources(step, filled):
        for unit in range(4):
            source = step * 4 + unit
            code = jnp.int32(0)
            for batch in range(NB):
                part = table[own, source * NB + batch] ^ (2 * rank)
                code = jnp.where(part < 2, 8 + 2 * batch + part, code)
            choice = lax.shift_right_logical(code, 1) & 3
            target = table[column, source * NB + choice] - column * col_blocks
            work[filled + 1] = source * 64 + (code & 1) * 32 + target * 2
            filled = filled + lax.shift_right_logical(code, 3)
        return filled

    filled = lax.fori_loop(0, sources // 4, list_sources, jnp.int32(0))
    work[0] = filled
    work[filled + 1] = work[jnp.maximum(filled, 1)]


def spread(row_params, col_params, basis):
    row_blocks = row_params.shape[0] // BLK

    def fill(params, slot, target, comp):
        upright = params[pl.ds(pl.multiple_of(slot * BLK, BLK), BLK), :]
        basis[target, comp] = jnp.broadcast_to(upright[:, comp : comp + 1], (BLK, LANES))

    for comp in range(4):
        for row in range(row_blocks):
            fill(row_params, row, row, comp)

        def fill_columns(step, carry):
            for unit in range(8):
                fill(col_params, 8 * step + unit, row_blocks + 8 * step + unit, comp)
            return carry

        lax.fori_loop(0, col_params.shape[0] // BLK // 8, fill_columns, 0)


def side_of(basis, slot):
    return lambda comp: basis[slot, comp]


def total_rows(array):
    return jnp.sum(array, axis=0, keepdims=True)


def decode(entry):
    half = entry & 1
    block = lax.shift_right_logical(entry, 1) & 15
    row = lax.shift_right_logical(entry, 5) & 1
    source = lax.shift_right_logical(entry, 6)
    return source, row, block, half


def values_of(side, point):
    offset = [point[comp] - side(comp) for comp in range(3)]
    distance = offset[0] * offset[0] + offset[1] * offset[1] + offset[2] * offset[2]
    return jnp.exp2(distance * side(3))


def over_pairs(work, handle, carry):
    filled = work[0]

    def pair(step, carry):
        entries = [(work[2 * step + unit + 1], 2 * step + unit < filled) for unit in range(2)]
        return handle(entries, carry)

    return lax.fori_loop(0, lax.shift_right_logical(filled + 1, 1), pair, carry)


def density_kernel(
    work, arrived, row_params, col_params, forward, backward, out, later, basis
):
    row_blocks = row_params.shape[0] // BLK
    spread(row_params, col_params, basis)
    out[...] = jnp.zeros_like(out)

    def partial_sums(entry):
        source, row, block, half = decode(entry)
        point = [arrived[source, pl.ds(half * 4 + comp, 1), :] for comp in range(3)]
        row_side = side_of(basis, row)
        col_side = side_of(basis, row_blocks + block)

        row_values = values_of(row_side, point)
        col_values = values_of(col_side, point)
        right = jnp.dot(
            backward[block, row], row_values.astype(jnp.bfloat16), preferred_element_type=jnp.float32
        )
        left = jnp.dot(
            forward[block, row], col_values.astype(jnp.bfloat16), preferred_element_type=jnp.float32
        )
        col_product = col_values * right
        col_slope = col_product * col_side(3)
        row_slope = row_values * left * row_side(3)
        slope = total_rows(row_slope + col_slope)
        sums = [total_rows(col_product)]
        for comp in range(3):
            moment = total_rows(row_slope * row_side(comp) + col_slope * col_side(comp))
            sums.append(SLOPE * (point[comp] * slope - moment))
        return source, half, sums

    def first_halves(entries, filled):
        for entry, real in entries:
            count = arrived[lax.shift_right_logical(entry, 6), 3:4, :][0, 0]
            later[filled + 1] = entry + 1
            filled = filled + jnp.where(jnp.logical_and(count > LANES, real), 1, 0)
        return halves(entries, filled)

    def halves(entries, carry):
        results = [partial_sums(entry) for entry, _ in entries]
        for source, half, sums in results:
            for comp in range(4):
                out[source, pl.ds(half * 4 + comp, 1), :] = sums[comp]
        return carry

    filled = over_pairs(work, first_halves, jnp.int32(0))
    later[0] = filled
    later[filled + 1] = later[jnp.maximum(filled, 1)]
    over_pairs(later, halves, 0)


def collect_kernel(slots, arrived, out):
    columns = slots.shape[0] // NB
    for batch in range(NB):
        total = arrived[slots[batch]]
        for column in range(1, columns):
            total = total + arrived[slots[column * NB + batch]]
        for copy in range(out.shape[0]):
            out[copy, batch] = total


def point_kernel(
    slots, counts, sums, weights, core, out, charge_out, energy_out, summed, tiles, scale
):
    columns = slots.shape[0] // NB
    for batch in range(NB):
        total = sums[0, batch]
        for column in range(1, sums.shape[0]):
            total = total + sums[column, batch]
        summed[pl.ds(batch * 8, 8), :] = total
    lane = lax.broadcasted_iota(jnp.int32, (1, LANES), 1)
    for batch in range(NB):
        for half in range(HALVES):
            place_row = pl.ds(batch * HALVES + half, 1)
            live = jnp.where(lane + half * LANES < counts[batch], 1.0, 0.0).astype(jnp.float32)
            scale[0, place_row, :] = live
            scale[1, place_row, :] = weights[pl.ds(batch, 1), pl.ds(half * LANES, LANES)]
            scale[2, place_row, :] = core[pl.ds(batch, 1), pl.ds(half * LANES, LANES)]
    live = scale[0]
    point_scale = scale[1] * live
    count_rows = NB * HALVES
    valence = live * summed[pl.ds(0, count_rows, stride=4), :]
    gradient = [live * summed[pl.ds(comp + 1, count_rows, stride=4), :] for comp in range(3)]
    grad_square = (
        gradient[0] * gradient[0] + gradient[1] * gradient[1] + gradient[2] * gradient[2]
    )
    total = valence + scale[2]
    root = jnp.sqrt(total * total + soft_square)
    regular = 0.5 * (total + root)
    third = jnp.exp(jnp.log(regular) * (1.0 / 3.0))
    four_thirds = regular * third
    scaled = grad_scale * four_thirds * four_thirds
    weighted = mu_coef * grad_square
    inverse = 1.0 / (kappa_pbe * scaled + weighted)
    fraction = scaled * inverse
    enhance = 1.0 + kappa_pbe - kappa_pbe * kappa_pbe * fraction
    energy = slater * four_thirds * enhance
    square = kappa_pbe * kappa_pbe * mu_coef
    deriv_sigma = slater * four_thirds * (square * fraction * inverse)
    enhance_slope = (
        -(kappa_pbe * kappa_pbe)
        * (weighted * inverse)
        * inverse
        * (grad_scale * (8.0 / 3.0) * four_thirds * third)
    )
    deriv_regular = slater * ((4.0 / 3.0) * third * enhance + four_thirds * enhance_slope)
    deriv_density = deriv_regular * (0.5 * (1.0 + total / root))
    fweight = point_scale * deriv_density
    factor = 2.0 * point_scale * deriv_sigma
    results = [fweight] + [factor * gradient[comp] for comp in range(3)]
    tiles[pl.ds(0, count_rows, stride=4), :] = results[0]
    for comp in range(3):
        tiles[pl.ds(comp + 1, count_rows, stride=4), :] = results[comp + 1]
    out[...] = jnp.zeros_like(out)
    for batch in range(NB):
        tile = tiles[pl.ds(batch * 8, 8), :]
        for column in range(columns):
            out[slots[column * NB + batch]] = tile
    scale[0] = valence
    scale[1] = point_scale * energy
    for batch in range(NB):
        for half in range(HALVES):
            charge_out[pl.ds(batch, 1), pl.ds(half * LANES, LANES)] = scale[
                0, pl.ds(batch * HALVES + half, 1), :
            ]
        energy_out[batch] = jnp.sum(scale[1, pl.ds(batch * HALVES, HALVES), :])


def potential_kernel(work, later, arrived, factors, row_params, col_params, out, basis):
    row_blocks = row_params.shape[0] // BLK
    spread(row_params, col_params, basis)
    out[...] = jnp.zeros_like(out)

    def tile_of(entry, real):
        source, row, block, half = decode(entry)
        keep = jnp.where(real, 1.0, 0.0).astype(jnp.float32)
        point = [arrived[source, pl.ds(half * 4 + comp, 1), :] for comp in range(3)]
        factor = [factors[source, pl.ds(half * 4 + comp, 1), :] * keep for comp in range(4)]
        push = [SLOPE * factor[comp + 1] for comp in range(3)]
        along_point = push[0] * point[0] + push[1] * point[1] + push[2] * point[2]

        def turn(side):
            along_centre = push[0] * side(0) + push[1] * side(1) + push[2] * side(2)
            return (along_point - along_centre) * side(3)
        row_side = side_of(basis, row)
        col_side = side_of(basis, row_blocks + block)

        row_values = values_of(row_side, point)
        col_values = values_of(col_side, point)
        row_across = row_values * turn(row_side)
        along = col_values * (factor[0] + turn(col_side))
        left_side = jnp.concatenate(
            [row_values.astype(jnp.bfloat16), row_across.astype(jnp.bfloat16)], axis=1
        )
        right_side = jnp.concatenate(
            [along.astype(jnp.bfloat16), col_values.astype(jnp.bfloat16)], axis=1
        )
        product = lax.dot_general(
            left_side,
            right_side,
            (((1,), (1,)), ((), ())),
            preferred_element_type=jnp.float32,
        )
        row_start = pl.multiple_of(row * BLK, BLK)
        col_start = pl.multiple_of(block * BLK, BLK)
        return row_start, col_start, product

    def handle(entries, carry):
        results = [tile_of(entry, real) for entry, real in entries]
        for row_start, col_start, product in results:
            place = (pl.ds(row_start, BLK), pl.ds(col_start, BLK))
            out[place] = out[place] + product
        return carry

    over_pairs(work, handle, 0)
    over_pairs(later, handle, 0)


def local(density, centres, exponents, coords, weights, core_density, counts, blocks):
    sources = lax.axis_size("grid")
    columns = lax.axis_size("col")
    rows, cols = density.shape
    points = coords.shape[2]
    f32 = jnp.float32
    params = pltpu.CompilerParams(vmem_limit_bytes=16 * 1024 * 1024)
    table = blocks.T
    shape = jax.ShapeDtypeStruct
    messages = shape((sources, 8, LANES), f32)
    tile_shape = shape((cols // BLK, rows // BLK, BLK, BLK), jnp.bfloat16)
    basis = pltpu.VMEM((rows // BLK + cols // BLK, 4, BLK, LANES), f32)
    listed = shape((sources + 8,), jnp.int32)

    outgoing, slots = pl.pallas_call(
        pack_kernel,
        out_shape=(messages, shape((columns * NB,), jnp.int32)),
        in_specs=[HBM, HBM, HBM],
        out_specs=(VMEM, SMEM),
        scratch_shapes=[
            pltpu.SMEM(table.shape, jnp.int32),
            pltpu.SMEM(counts.shape, jnp.int32),
            pltpu.VMEM((3, NB, points), f32),
            pltpu.VMEM((NB, 8, LANES), f32),
            pltpu.SemaphoreType.DMA((3,)),
        ],
        compiler_params=params,
        name="pack",
    )(
        *[
            pltpu.with_memory_space_constraint(array, pltpu.HBM)
            for array in (table, counts, coords.transpose(1, 0, 2))
        ]
    )
    arrived = lax.all_to_all(outgoing, "grid", split_axis=0, concat_axis=0, tiled=True)
    row_params, col_params, forward, backward, work = pl.pallas_call(
        partial(prepare_kernel, group=sources // columns),
        out_shape=(shape((rows, 8), f32), shape((cols, 8), f32), tile_shape, tile_shape, listed),
        in_specs=[SMEM, VMEM, VMEM, VMEM],
        out_specs=(VMEM,) * 4 + (SMEM,),
        scratch_shapes=[pltpu.VMEM((8, LANES), f32)],
        compiler_params=params,
        name="prepare",
    )(table, centres, exponents.reshape(-1, LANES), density)
    partials, later = pl.pallas_call(
        density_kernel,
        out_shape=(messages, listed),
        in_specs=[SMEM] + [VMEM] * 5,
        out_specs=(VMEM, SMEM),
        scratch_shapes=[basis],
        compiler_params=params,
        name="density",
    )(work, arrived, row_params, col_params, forward, backward)
    returned = lax.all_to_all(partials, "grid", split_axis=0, concat_axis=0, tiled=True)
    copies = pl.pallas_call(
        collect_kernel,
        out_shape=shape((columns, NB, 8, LANES), f32),
        in_specs=[SMEM, VMEM],
        out_specs=VMEM,
        compiler_params=params,
        name="collect",
    )(slots, returned)
    everything = lax.all_to_all(copies, "col", split_axis=0, concat_axis=0, tiled=True)
    sending, orbital_charge_samples, xc_batch_amounts = pl.pallas_call(
        point_kernel,
        out_shape=(messages, shape((NB, points), f32), shape((NB,), f32)),
        in_specs=[SMEM, SMEM, VMEM, VMEM, VMEM],
        out_specs=(VMEM, VMEM, SMEM),
        scratch_shapes=[
            pltpu.VMEM((NB * 8, LANES), f32),
            pltpu.VMEM((NB * 8, LANES), f32),
            pltpu.VMEM((3, 8, LANES), f32),
        ],
        compiler_params=params,
        name="points",
    )(slots, counts, everything, weights, core_density)
    factors = lax.all_to_all(sending, "grid", split_axis=0, concat_axis=0, tiled=True)
    potential_matrix_xc = pl.pallas_call(
        potential_kernel,
        out_shape=shape((rows, cols), f32),
        in_specs=[SMEM, SMEM] + [VMEM] * 4,
        out_specs=VMEM,
        scratch_shapes=[basis],
        compiler_params=params,
        name="potential",
    )(work, later, arrived, factors, row_params, col_params)
    return (potential_matrix_xc, orbital_charge_samples, xc_batch_amounts)


def solution(mesh):
    return jax.shard_map(
        local,
        mesh=mesh,
        in_specs=(
            P("grid", "col"),
            P(),
            P(),
            P("grid", None, None),
            P("grid", None),
            P("grid", None),
            P("grid"),
            P(),
        ),
        out_specs=(P("grid", "col"), P("grid", None), P("grid")),
        check_vma=False,
    )
```

```python
from functools import partial
import math

import jax
import jax.numpy as jnp
from jax import lax
from jax.experimental import pallas as pl
from jax.experimental.pallas import tpu as pltpu
from jax.sharding import PartitionSpec as P

BLK = 128
NB = 4
LANES = 128
HALVES = 2

kappa_pbe = 0.804
mu_coef = 0.2195
slater = -0.7385587663820224
grad_scale = 4.0 * (3.0 * math.pi**2) ** (2.0 / 3.0)
soft_square = 0.25

SMEM = pl.BlockSpec(memory_space=pltpu.SMEM)
VMEM = pl.BlockSpec(memory_space=pltpu.VMEM)


PIECES = 3
GROUP = 4
LOG2E = math.log2(math.e)
SLOPE = 2.0 * math.log(2.0)
HBM = pl.BlockSpec(memory_space=pltpu.HBM)


def pack_kernel(table_hbm, counts_hbm, coords_hbm, out, slots, table, counts, coords, tiles, sems):
    copies = [
        pltpu.make_async_copy(source, target, sems.at[index])
        for index, (source, target) in enumerate(
            [(table_hbm, table), (counts_hbm, counts), (coords_hbm, coords)]
        )
    ]
    for copy in copies:
        copy.start()
    first = lax.axis_index("grid") * NB
    columns = table.shape[0]
    out[...] = jnp.zeros_like(out)
    for copy in copies:
        copy.wait()
    for batch in range(NB):
        count = jnp.full((1, LANES), counts[batch].astype(jnp.float32), jnp.float32)
        for half in range(HALVES):
            for comp in range(3):
                tiles[batch, pl.ds(half * 4 + comp, 1), :] = coords[
                    comp, pl.ds(batch, 1), pl.ds(half * LANES, LANES)
                ]
            tiles[batch, pl.ds(half * 4 + 3, 1), :] = count
    for batch in range(NB):
        tile = tiles[batch]
        for column in range(columns):
            slot = lax.shift_right_logical(table[column, first + batch], 1)
            slots[column * NB + batch] = slot
            out[slot] = tile


def prepare_kernel(table, centres, exponents, density, pieces, forward, backward, work, tile, *, group):
    rank = lax.axis_index("grid")
    column = lax.axis_index("col")
    own = rank // group
    row_blocks = density.shape[0] // BLK
    col_blocks = density.shape[1] // BLK
    sources = table.shape[1] // NB
    tile[...] = jnp.zeros_like(tile)

    def fill(block, slot):
        start = pl.multiple_of(block * BLK, BLK)
        tile[pl.ds(0, 3), :] = centres[:, pl.ds(start, BLK)]
        tile[pl.ds(3, 1), :] = exponents[pl.ds(block, 1), :] * (-LOG2E)
        rest = tile[pl.ds(0, 8), :]
        for index in range(PIECES):
            piece = rest.astype(jnp.bfloat16).astype(jnp.float32)
            tile[pl.ds((index + 1) * 8, 8), :] = piece
            rest = rest - piece
        pieces[slot] = tile[pl.ds(8, BLK), :].astype(jnp.bfloat16).T

    for slot in range(row_blocks):
        fill(rank * row_blocks + slot, slot)

    def fill_column(slot, carry):
        fill(column * col_blocks + slot, row_blocks + slot)
        start = pl.multiple_of(slot * BLK, BLK)
        for row in range(row_blocks):
            piece = density[pl.ds(row * BLK, BLK), pl.ds(start, BLK)]
            forward[slot, row] = piece
            backward[slot, row] = piece.T
        return carry

    lax.fori_loop(0, col_blocks, fill_column, 0)

    def list_sources(step, filled):
        for unit in range(4):
            source = step * 4 + unit
            code = jnp.int32(0)
            for batch in range(NB):
                part = table[own, source * NB + batch] ^ (2 * rank)
                code = jnp.where(part < 2, 8 + 2 * batch + part, code)
            choice = lax.shift_right_logical(code, 1) & 3
            target = table[column, source * NB + choice] - column * col_blocks
            work[filled + 1] = source * 64 + (code & 1) * 32 + target * 2
            filled = filled + lax.shift_right_logical(code, 3)
        return filled

    filled = lax.fori_loop(0, sources // 4, list_sources, jnp.int32(0))
    close_list(work, filled)


def spread(pieces, basis):
    index = lax.broadcasted_iota(jnp.int32, (BLK, 4 * LANES), 0)
    lane = lax.broadcasted_iota(jnp.int32, (BLK, 4 * LANES), 1)
    picked = jnp.logical_and(index < 8 * PIECES, (index & 7) == lax.shift_right_logical(lane, 7))
    chooser = jnp.where(picked, 1.0, 0.0).astype(jnp.bfloat16)

    def fill(slot, carry):
        wide = jnp.dot(pieces[slot], chooser, preferred_element_type=jnp.float32)
        for comp in range(4):
            basis[slot, comp] = wide[:, comp * LANES : (comp + 1) * LANES]
        return carry

    lax.fori_loop(0, pieces.shape[0], fill, 0, unroll=2)


def side_of(basis, slot):
    return lambda comp: basis[slot, comp]


def total_rows(array):
    return jnp.sum(array, axis=0, keepdims=True)


def decode(entry):
    half = entry & 1
    block = lax.shift_right_logical(entry, 1) & 15
    row = lax.shift_right_logical(entry, 5) & 1
    source = lax.shift_right_logical(entry, 6)
    return source, row, block, half


def values_of(side, point):
    offset = [point[comp] - side(comp) for comp in range(3)]
    distance = offset[0] * offset[0] + offset[1] * offset[1] + offset[2] * offset[2]
    return jnp.exp2(distance * side(3))


def close_list(work, filled):
    work[0] = filled
    for unit in range(1, GROUP):
        work[filled + unit] = work[jnp.maximum(filled, 1)]


def over_groups(work, handle, carry):
    filled = work[0]

    def group(step, carry):
        entries = [
            (work[GROUP * step + unit + 1], GROUP * step + unit < filled) for unit in range(GROUP)
        ]
        return handle(entries, carry)

    return lax.fori_loop(0, (filled + GROUP - 1) // GROUP, group, carry)


def density_kernel(
    work, arrived, pieces, forward, backward, out, later, basis
):
    row_blocks = forward.shape[1]
    spread(pieces, basis)
    out[...] = jnp.zeros_like(out)

    def partial_sums(entry):
        source, row, block, half = decode(entry)
        point = [arrived[source, pl.ds(half * 4 + comp, 1), :] for comp in range(3)]
        row_side = side_of(basis, row)
        col_side = side_of(basis, row_blocks + block)

        row_values = values_of(row_side, point)
        col_values = values_of(col_side, point)
        right = jnp.dot(
            backward[block, row], row_values.astype(jnp.bfloat16), preferred_element_type=jnp.float32
        )
        left = jnp.dot(
            forward[block, row], col_values.astype(jnp.bfloat16), preferred_element_type=jnp.float32
        )
        col_product = col_values * right
        col_slope = col_product * col_side(3)
        row_slope = row_values * left * row_side(3)
        slope = total_rows(row_slope + col_slope)
        sums = [total_rows(col_product)]
        for comp in range(3):
            moment = total_rows(row_slope * row_side(comp) + col_slope * col_side(comp))
            sums.append(SLOPE * (point[comp] * slope - moment))
        return source, half, sums

    def first_halves(entries, filled):
        for entry, real in entries:
            count = arrived[lax.shift_right_logical(entry, 6), 3:4, :][0, 0]
            later[filled + 1] = entry + 1
            filled = filled + jnp.where(jnp.logical_and(count > LANES, real), 1, 0)
        return halves(entries, filled)

    def halves(entries, carry):
        results = [partial_sums(entry) for entry, _ in entries]
        for source, half, sums in results:
            for comp in range(4):
                out[source, pl.ds(half * 4 + comp, 1), :] = sums[comp]
        return carry

    filled = over_groups(work, first_halves, jnp.int32(0))
    close_list(later, filled)
    over_groups(later, halves, 0)


def collect_kernel(slots, arrived, out):
    columns = slots.shape[0] // NB
    for batch in range(NB):
        total = arrived[slots[batch]]
        for column in range(1, columns):
            total = total + arrived[slots[column * NB + batch]]
        for copy in range(out.shape[0]):
            out[copy, batch] = total


def point_kernel(
    slots, counts, sums, weights, core, out, charge_out, energy_out, summed, tiles, scale
):
    columns = slots.shape[0] // NB
    for batch in range(NB):
        total = sums[0, batch]
        for column in range(1, sums.shape[0]):
            total = total + sums[column, batch]
        summed[pl.ds(batch * 8, 8), :] = total
    lane = lax.broadcasted_iota(jnp.int32, (1, LANES), 1)
    for batch in range(NB):
        for half in range(HALVES):
            place_row = pl.ds(batch * HALVES + half, 1)
            live = jnp.where(lane + half * LANES < counts[batch], 1.0, 0.0).astype(jnp.float32)
            scale[0, place_row, :] = live
            scale[1, place_row, :] = weights[pl.ds(batch, 1), pl.ds(half * LANES, LANES)]
            scale[2, place_row, :] = core[pl.ds(batch, 1), pl.ds(half * LANES, LANES)]
    live = scale[0]
    point_scale = scale[1] * live
    count_rows = NB * HALVES
    valence = live * summed[pl.ds(0, count_rows, stride=4), :]
    gradient = [live * summed[pl.ds(comp + 1, count_rows, stride=4), :] for comp in range(3)]
    grad_square = (
        gradient[0] * gradient[0] + gradient[1] * gradient[1] + gradient[2] * gradient[2]
    )
    total = valence + scale[2]
    root = jnp.sqrt(total * total + soft_square)
    regular = 0.5 * (total + root)
    third = jnp.exp(jnp.log(regular) * (1.0 / 3.0))
    four_thirds = regular * third
    scaled = grad_scale * four_thirds * four_thirds
    weighted = mu_coef * grad_square
    inverse = 1.0 / (kappa_pbe * scaled + weighted)
    fraction = scaled * inverse
    enhance = 1.0 + kappa_pbe - kappa_pbe * kappa_pbe * fraction
    energy = slater * four_thirds * enhance
    square = kappa_pbe * kappa_pbe * mu_coef
    deriv_sigma = slater * four_thirds * (square * fraction * inverse)
    enhance_slope = (
        -(kappa_pbe * kappa_pbe)
        * (weighted * inverse)
        * inverse
        * (grad_scale * (8.0 / 3.0) * four_thirds * third)
    )
    deriv_regular = slater * ((4.0 / 3.0) * third * enhance + four_thirds * enhance_slope)
    deriv_density = deriv_regular * (0.5 * (1.0 + total / root))
    fweight = point_scale * deriv_density
    factor = 2.0 * point_scale * deriv_sigma
    results = [fweight] + [factor * gradient[comp] for comp in range(3)]
    tiles[pl.ds(0, count_rows, stride=4), :] = results[0]
    for comp in range(3):
        tiles[pl.ds(comp + 1, count_rows, stride=4), :] = results[comp + 1]
    out[...] = jnp.zeros_like(out)
    for batch in range(NB):
        tile = tiles[pl.ds(batch * 8, 8), :]
        for column in range(columns):
            out[slots[column * NB + batch]] = tile
    scale[0] = valence
    scale[1] = point_scale * energy
    for batch in range(NB):
        for half in range(HALVES):
            charge_out[pl.ds(batch, 1), pl.ds(half * LANES, LANES)] = scale[
                0, pl.ds(batch * HALVES + half, 1), :
            ]
        energy_out[batch] = jnp.sum(scale[1, pl.ds(batch * HALVES, HALVES), :])


def potential_kernel(work, later, arrived, factors, pieces, out, basis):
    row_blocks = out.shape[0] // BLK
    spread(pieces, basis)
    out[...] = jnp.zeros_like(out)

    def tile_of(entry, real):
        source, row, block, half = decode(entry)
        keep = jnp.where(real, 1.0, 0.0).astype(jnp.float32)
        point = [arrived[source, pl.ds(half * 4 + comp, 1), :] for comp in range(3)]
        factor = [factors[source, pl.ds(half * 4 + comp, 1), :] * keep for comp in range(4)]
        push = [SLOPE * factor[comp + 1] for comp in range(3)]
        along_point = push[0] * point[0] + push[1] * point[1] + push[2] * point[2]

        def turn(side):
            along_centre = push[0] * side(0) + push[1] * side(1) + push[2] * side(2)
            return (along_point - along_centre) * side(3)
        row_side = side_of(basis, row)
        col_side = side_of(basis, row_blocks + block)

        row_values = values_of(row_side, point)
        col_values = values_of(col_side, point)
        row_across = row_values * turn(row_side)
        along = col_values * (factor[0] + turn(col_side))
        left_side = jnp.concatenate(
            [row_values.astype(jnp.bfloat16), row_across.astype(jnp.bfloat16)], axis=1
        )
        right_side = jnp.concatenate(
            [along.astype(jnp.bfloat16), col_values.astype(jnp.bfloat16)], axis=1
        )
        product = lax.dot_general(
            left_side,
            right_side,
            (((1,), (1,)), ((), ())),
            preferred_element_type=jnp.float32,
        )
        row_start = pl.multiple_of(row * BLK, BLK)
        col_start = pl.multiple_of(block * BLK, BLK)
        return row_start, col_start, product

    def handle(entries, carry):
        results = [tile_of(entry, real) for entry, real in entries]
        for row_start, col_start, product in results:
            place = (pl.ds(row_start, BLK), pl.ds(col_start, BLK))
            out[place] = out[place] + product
        return carry

    over_groups(work, handle, 0)
    over_groups(later, handle, 0)


def local(density, centres, exponents, coords, weights, core_density, counts, blocks):
    sources = lax.axis_size("grid")
    columns = lax.axis_size("col")
    rows, cols = density.shape
    points = coords.shape[2]
    f32 = jnp.float32
    params = pltpu.CompilerParams(vmem_limit_bytes=16 * 1024 * 1024)
    table = blocks.T
    shape = jax.ShapeDtypeStruct
    messages = shape((sources, 8, LANES), f32)
    tile_shape = shape((cols // BLK, rows // BLK, BLK, BLK), jnp.bfloat16)
    basis = pltpu.VMEM((rows // BLK + cols // BLK, 4, BLK, LANES), f32)
    listed = shape((sources + 8,), jnp.int32)

    outgoing, slots = pl.pallas_call(
        pack_kernel,
        out_shape=(messages, shape((columns * NB,), jnp.int32)),
        in_specs=[HBM, HBM, HBM],
        out_specs=(VMEM, SMEM),
        scratch_shapes=[
            pltpu.SMEM(table.shape, jnp.int32),
            pltpu.SMEM(counts.shape, jnp.int32),
            pltpu.VMEM((3, NB, points), f32),
            pltpu.VMEM((NB, 8, LANES), f32),
            pltpu.SemaphoreType.DMA((3,)),
        ],
        compiler_params=params,
        name="pack",
    )(
        *[
            pltpu.with_memory_space_constraint(array, pltpu.HBM)
            for array in (table, counts, coords.transpose(1, 0, 2))
        ]
    )
    arrived = lax.all_to_all(outgoing, "grid", split_axis=0, concat_axis=0, tiled=True)
    pieces, forward, backward, work = pl.pallas_call(
        partial(prepare_kernel, group=sources // columns),
        out_shape=(
            shape((rows // BLK + cols // BLK, BLK, BLK), jnp.bfloat16),
            tile_shape,
            tile_shape,
            listed,
        ),
        in_specs=[SMEM, VMEM, VMEM, VMEM],
        out_specs=(VMEM,) * 3 + (SMEM,),
        scratch_shapes=[pltpu.VMEM((8 + BLK, LANES), f32)],
        compiler_params=params,
        name="prepare",
    )(table, centres, exponents.reshape(-1, LANES), density)
    partials, later = pl.pallas_call(
        density_kernel,
        out_shape=(messages, listed),
        in_specs=[SMEM] + [VMEM] * 4,
        out_specs=(VMEM, SMEM),
        scratch_shapes=[basis],
        compiler_params=params,
        name="density",
    )(work, arrived, pieces, forward, backward)
    returned = lax.all_to_all(partials, "grid", split_axis=0, concat_axis=0, tiled=True)
    copies = pl.pallas_call(
        collect_kernel,
        out_shape=shape((columns, NB, 8, LANES), f32),
        in_specs=[SMEM, VMEM],
        out_specs=VMEM,
        compiler_params=params,
        name="collect",
    )(slots, returned)
    everything = lax.all_to_all(copies, "col", split_axis=0, concat_axis=0, tiled=True)
    sending, orbital_charge_samples, xc_batch_amounts = pl.pallas_call(
        point_kernel,
        out_shape=(messages, shape((NB, points), f32), shape((NB,), f32)),
        in_specs=[SMEM, SMEM, VMEM, VMEM, VMEM],
        out_specs=(VMEM, VMEM, SMEM),
        scratch_shapes=[
            pltpu.VMEM((NB * 8, LANES), f32),
            pltpu.VMEM((NB * 8, LANES), f32),
            pltpu.VMEM((3, 8, LANES), f32),
        ],
        compiler_params=params,
        name="points",
    )(slots, counts, everything, weights, core_density)
    factors = lax.all_to_all(sending, "grid", split_axis=0, concat_axis=0, tiled=True)
    potential_matrix_xc = pl.pallas_call(
        potential_kernel,
        out_shape=shape((rows, cols), f32),
        in_specs=[SMEM, SMEM] + [VMEM] * 3,
        out_specs=VMEM,
        scratch_shapes=[basis],
        compiler_params=params,
        name="potential",
    )(work, later, arrived, factors, pieces)
    return (potential_matrix_xc, orbital_charge_samples, xc_batch_amounts)


def solution(mesh):
    return jax.shard_map(
        local,
        mesh=mesh,
        in_specs=(
            P("grid", "col"),
            P(),
            P(),
            P("grid", None, None),
            P("grid", None),
            P("grid", None),
            P("grid"),
            P(),
        ),
        out_specs=(P("grid", "col"), P("grid", None), P("grid")),
        check_vma=False,
    )
```

```python
from functools import partial
import math

import jax
import jax.numpy as jnp
from jax import lax
from jax.experimental import pallas as pl
from jax.experimental.pallas import tpu as pltpu
from jax.sharding import PartitionSpec as P

BLK = 128
NB = 4
LANES = 128
HALVES = 2

kappa_pbe = 0.804
mu_coef = 0.2195
slater = -0.7385587663820224
grad_scale = 4.0 * (3.0 * math.pi**2) ** (2.0 / 3.0)
soft_square = 0.25

SMEM = pl.BlockSpec(memory_space=pltpu.SMEM)
VMEM = pl.BlockSpec(memory_space=pltpu.VMEM)


PIECES = 3
GROUP = 4
REAL = 1 << 16
FAR = 64.0
LOG2E = math.log2(math.e)
SLOPE = 2.0 * math.log(2.0)
HBM = pl.BlockSpec(memory_space=pltpu.HBM)


def start_all(pairs, sems):
    copies = [
        pltpu.make_async_copy(source, target, sems.at[index])
        for index, (source, target) in enumerate(pairs)
    ]
    for copy in copies:
        copy.start()
    return copies


def pack_kernel(table_hbm, counts_hbm, coords_hbm, out, slots, table, counts, coords, sems):
    copies = start_all([(table_hbm, table), (counts_hbm, counts), (coords_hbm, coords)], sems)
    first = lax.axis_index("grid") * NB
    columns = table.shape[0]
    points = coords.shape[2]
    lane = lax.broadcasted_iota(jnp.int32, (1, points), 1)
    for copy in copies:
        copy.wait()
    for batch in range(NB):
        live = lane < counts[batch]
        message = jnp.concatenate(
            [jnp.where(live, coords[comp, pl.ds(batch, 1), :], FAR) for comp in range(3)], axis=1
        )
        for column in range(columns):
            slot = lax.shift_right_logical(table[column, first + batch], 1)
            slots[column * NB + batch] = slot
            out[slot] = message


def prepare_kernel(*refs, group):
    hbm, (pieces, forward, backward, scale, work) = refs[:7], refs[7:12]
    table, counts, centres, exponents, weights, core, density = refs[12:19]
    tile, sems = refs[19:]
    copies = start_all(list(zip(hbm, refs[12:19])), sems)
    rank = lax.axis_index("grid")
    column = lax.axis_index("col")
    own = rank // group
    row_blocks = density.shape[0] // BLK
    col_blocks = density.shape[1] // BLK
    sources = table.shape[1] // NB
    for copy in copies[:2]:
        copy.wait()

    def list_sources(step, filled):
        for unit in range(4):
            source = step * 4 + unit
            code = jnp.int32(0)
            for batch in range(NB):
                part = table[own, source * NB + batch] ^ (2 * rank)
                code = jnp.where(part < 2, 8 + 2 * batch + part, code)
            choice = lax.shift_right_logical(code, 1) & 3
            target = table[column, source * NB + choice] - column * col_blocks
            work[filled + 1] = source * 64 + (code & 1) * 32 + target * 2
            filled = filled + lax.shift_right_logical(code, 3)
        return filled

    filled = lax.fori_loop(0, sources // 4, list_sources, jnp.int32(0))
    close_list(work, filled)

    for copy in copies[4:6]:
        copy.wait()
    lane = lax.broadcasted_iota(jnp.int32, (1, LANES), 1)
    for batch in range(NB):
        for half in range(HALVES):
            place = pl.ds(batch * HALVES + half, 1)
            part = (pl.ds(batch, 1), pl.ds(half * LANES, LANES))
            live = jnp.where(lane + half * LANES < counts[batch], 1.0, 0.0).astype(jnp.float32)
            scale[0, place, :] = live
            scale[1, place, :] = weights[part] * live
            scale[2, place, :] = core[part]

    tile[...] = jnp.zeros_like(tile)

    def fill(block, slot):
        start = pl.multiple_of(block * BLK, BLK)
        tile[pl.ds(0, 3), :] = centres[:, pl.ds(start, BLK)]
        tile[pl.ds(3, 1), :] = exponents[pl.ds(block, 1), :] * (-LOG2E)
        rest = tile[pl.ds(0, 8), :]
        for index in range(PIECES):
            piece = rest.astype(jnp.bfloat16).astype(jnp.float32)
            tile[pl.ds((index + 1) * 8, 8), :] = piece
            rest = rest - piece
        pieces[slot] = tile[pl.ds(8, BLK), :].astype(jnp.bfloat16).T

    for copy in copies[2:4]:
        copy.wait()
    for slot in range(row_blocks):
        fill(rank * row_blocks + slot, slot)

    def fill_column(slot, carry):
        fill(column * col_blocks + slot, row_blocks + slot)
        start = pl.multiple_of(slot * BLK, BLK)
        for row in range(row_blocks):
            piece = density[pl.ds(row * BLK, BLK), pl.ds(start, BLK)]
            forward[slot, row] = piece
            backward[slot, row] = piece.T
        return carry

    copies[6].wait()
    lax.fori_loop(0, col_blocks, fill_column, 0)


def spread(pieces, basis):
    index = lax.broadcasted_iota(jnp.int32, (BLK, 4 * LANES), 0)
    lane = lax.broadcasted_iota(jnp.int32, (BLK, 4 * LANES), 1)
    picked = jnp.logical_and(index < 8 * PIECES, (index & 7) == lax.shift_right_logical(lane, 7))
    chooser = jnp.where(picked, 1.0, 0.0).astype(jnp.bfloat16)

    def fill(slot, carry):
        wide = jnp.dot(pieces[slot], chooser, preferred_element_type=jnp.float32)
        for comp in range(4):
            basis[slot, comp] = wide[:, comp * LANES : (comp + 1) * LANES]
        return carry

    lax.fori_loop(0, pieces.shape[0], fill, 0, unroll=2)


def side_of(basis, slot):
    return lambda comp: basis[slot, comp]


def total_rows(array):
    return jnp.sum(array, axis=0, keepdims=True)


def decode(entry):
    half = entry & 1
    block = lax.shift_right_logical(entry, 1) & 15
    row = lax.shift_right_logical(entry, 5) & 1
    source = lax.shift_right_logical(entry, 6) & 1023
    return source, row, block, half


def point_of(arrived, source, half):
    points = arrived.shape[2] // 3
    return [
        arrived[source, :, pl.ds(pl.multiple_of(comp * points + half * LANES, LANES), LANES)]
        for comp in range(3)
    ]


def values_of(side, point):
    offset = [point[comp] - side(comp) for comp in range(3)]
    distance = offset[0] * offset[0] + offset[1] * offset[1] + offset[2] * offset[2]
    return jnp.exp2(distance * side(3))


def close_list(work, filled):
    work[0] = filled
    for unit in range(1, GROUP):
        work[filled + unit] = work[jnp.maximum(filled, 1)]


def groups_of(work):
    return (work[0] + GROUP - 1) // GROUP


def density_kernel(
    work, arrived, pieces, forward, backward, out, done, kept, later, basis, hold, sems
):
    row_blocks = forward.shape[1]
    spread(pieces, basis)
    out[...] = jnp.zeros_like(out)

    def partial_sums(entry):
        source, row, block, half = decode(entry)
        point = point_of(arrived, source, half)
        row_side = side_of(basis, row)
        col_side = side_of(basis, row_blocks + block)

        row_values = values_of(row_side, point)
        col_values = values_of(col_side, point)
        right = jnp.dot(
            backward[block, row], row_values.astype(jnp.bfloat16), preferred_element_type=jnp.float32
        )
        left = jnp.dot(
            forward[block, row], col_values.astype(jnp.bfloat16), preferred_element_type=jnp.float32
        )
        col_product = col_values * right
        col_slope = col_product * col_side(3)
        row_slope = row_values * left * row_side(3)
        slope = total_rows(row_slope + col_slope)
        sums = [total_rows(col_product)]
        for comp in range(3):
            moment = total_rows(row_slope * row_side(comp) + col_slope * col_side(comp))
            sums.append(SLOPE * (point[comp] * slope - moment))
        return source, half, sums, row_values, col_values

    def write_back(index):
        slot = index & 1
        return pltpu.make_async_copy(hold.at[slot], kept.at[index], sems.at[slot])

    def group(work, step, index):
        @pl.when(index >= 2)
        def _():
            write_back(index - 2).wait()

        entries = [work[GROUP * step + unit + 1] for unit in range(GROUP)]
        results = [partial_sums(entry) for entry in entries]
        for unit, (source, half, sums, row_values, col_values) in enumerate(results):
            for comp in range(4):
                out[source, pl.ds(half * 4 + comp, 1), :] = sums[comp]
            hold[index & 1, unit, 0] = row_values
            hold[index & 1, unit, 1] = col_values
            real = jnp.where(GROUP * step + unit < work[0], REAL, 0)
            done[GROUP * index + unit + 1] = entries[unit] + real
        write_back(index).start()

    def first_halves(step, filled):
        for unit in range(GROUP):
            entry = work[GROUP * step + unit + 1]
            beyond = point_of(arrived, decode(entry)[0], 1)[0][0, 0]
            later[filled + 1] = entry + 1
            real = jnp.logical_and(beyond < FAR, GROUP * step + unit < work[0])
            filled = filled + jnp.where(real, 1, 0)
        group(work, step, step)
        return filled

    firsts = groups_of(work)
    filled = lax.fori_loop(0, firsts, first_halves, jnp.int32(0))
    close_list(later, filled)

    def second_halves(step, carry):
        group(later, step, firsts + step)
        return carry

    total = firsts + groups_of(later)
    lax.fori_loop(0, groups_of(later), second_halves, 0)
    done[0] = total
    for back in (2, 1):

        @pl.when(total >= back)
        def _():
            write_back(total - back).wait()


def collect_kernel(slots, arrived, out):
    columns = slots.shape[0] // NB
    for batch in range(NB):
        total = arrived[slots[batch]]
        for column in range(1, columns):
            total = total + arrived[slots[column * NB + batch]]
        for copy in range(out.shape[0]):
            out[copy, batch] = total


def point_kernel(
    slots, sums, scale, out, charge_out, energy_out, summed, tiles, results_at
):
    columns = slots.shape[0] // NB
    for batch in range(NB):
        total = sums[0, batch]
        for column in range(1, sums.shape[0]):
            total = total + sums[column, batch]
        summed[pl.ds(batch * 8, 8), :] = total
    live = scale[0]
    point_scale = scale[1]
    count_rows = NB * HALVES
    valence = live * summed[pl.ds(0, count_rows, stride=4), :]
    gradient = [live * summed[pl.ds(comp + 1, count_rows, stride=4), :] for comp in range(3)]
    grad_square = (
        gradient[0] * gradient[0] + gradient[1] * gradient[1] + gradient[2] * gradient[2]
    )
    total = valence + scale[2]
    root = jnp.sqrt(total * total + soft_square)
    regular = 0.5 * (total + root)
    third = jnp.exp(jnp.log(regular) * (1.0 / 3.0))
    four_thirds = regular * third
    scaled = grad_scale * four_thirds * four_thirds
    weighted = mu_coef * grad_square
    inverse = 1.0 / (kappa_pbe * scaled + weighted)
    fraction = scaled * inverse
    enhance = 1.0 + kappa_pbe - kappa_pbe * kappa_pbe * fraction
    energy = slater * four_thirds * enhance
    square = kappa_pbe * kappa_pbe * mu_coef
    deriv_sigma = slater * four_thirds * (square * fraction * inverse)
    enhance_slope = (
        -(kappa_pbe * kappa_pbe)
        * (weighted * inverse)
        * inverse
        * (grad_scale * (8.0 / 3.0) * four_thirds * third)
    )
    deriv_regular = slater * ((4.0 / 3.0) * third * enhance + four_thirds * enhance_slope)
    deriv_density = deriv_regular * (0.5 * (1.0 + total / root))
    fweight = point_scale * deriv_density
    factor = 2.0 * point_scale * deriv_sigma
    results = [fweight] + [factor * gradient[comp] for comp in range(3)]
    for comp in range(4):
        tiles[pl.ds(comp, count_rows, stride=4), :] = results[comp]
    for batch in range(NB):
        tile = tiles[pl.ds(batch * 8, 8), :]
        for column in range(columns):
            out[slots[column * NB + batch]] = tile
    results_at[0] = valence
    results_at[1] = point_scale * energy
    for batch in range(NB):
        for half in range(HALVES):
            charge_out[pl.ds(batch, 1), pl.ds(half * LANES, LANES)] = results_at[
                0, pl.ds(batch * HALVES + half, 1), :
            ]
        energy_out[batch] = jnp.sum(results_at[1, pl.ds(batch * HALVES, HALVES), :])


def potential_kernel(done, arrived, factors, pieces, kept, out, basis, held, sems):
    row_blocks = out.shape[0] // BLK
    total = done[0]

    def fetch(index):
        slot = index & 1
        return pltpu.make_async_copy(kept.at[index], held.at[slot], sems.at[slot])

    @pl.when(total > 0)
    def _():
        fetch(0).start()

    spread(pieces, basis)
    out[...] = jnp.zeros_like(out)

    def tile_of(entry, row_values, col_values):
        source, row, block, half = decode(entry)
        keep = jnp.where(entry >= REAL, 1.0, 0.0).astype(jnp.float32)
        point = point_of(arrived, source, half)
        factor = [factors[source, pl.ds(half * 4 + comp, 1), :] * keep for comp in range(4)]
        push = [SLOPE * factor[comp + 1] for comp in range(3)]
        along_point = push[0] * point[0] + push[1] * point[1] + push[2] * point[2]

        def turn(side):
            along_centre = push[0] * side(0) + push[1] * side(1) + push[2] * side(2)
            return (along_point - along_centre) * side(3)
        row_side = side_of(basis, row)
        col_side = side_of(basis, row_blocks + block)

        row_across = row_values * turn(row_side)
        along = col_values * (factor[0] + turn(col_side))
        left_side = jnp.concatenate(
            [row_values.astype(jnp.bfloat16), row_across.astype(jnp.bfloat16)], axis=1
        )
        right_side = jnp.concatenate(
            [along.astype(jnp.bfloat16), col_values.astype(jnp.bfloat16)], axis=1
        )
        product = lax.dot_general(
            left_side,
            right_side,
            (((1,), (1,)), ((), ())),
            preferred_element_type=jnp.float32,
        )
        row_start = pl.multiple_of(row * BLK, BLK)
        col_start = pl.multiple_of(block * BLK, BLK)
        return row_start, col_start, product

    def group(index, carry):
        @pl.when(index + 1 < total)
        def _():
            fetch(index + 1).start()

        fetch(index).wait()
        results = [
            tile_of(
                done[GROUP * index + unit + 1], held[index & 1, unit, 0], held[index & 1, unit, 1]
            )
            for unit in range(GROUP)
        ]
        for row_start, col_start, product in results:
            place = (pl.ds(row_start, BLK), pl.ds(col_start, BLK))
            out[place] = out[place] + product
        return carry

    lax.fori_loop(0, total, group, 0)


def local(density, centres, exponents, coords, weights, core_density, counts, blocks):
    sources = lax.axis_size("grid")
    columns = lax.axis_size("col")
    rows, cols = density.shape
    points = coords.shape[2]
    f32 = jnp.float32
    params = pltpu.CompilerParams(vmem_limit_bytes=16 * 1024 * 1024)
    table = blocks.T
    shape = jax.ShapeDtypeStruct
    messages = shape((sources, 8, LANES), f32)
    tile_shape = shape((cols // BLK, rows // BLK, BLK, BLK), jnp.bfloat16)
    basis = pltpu.VMEM((rows // BLK + cols // BLK, 4, BLK, LANES), f32)
    listed = shape((sources + 8,), jnp.int32)

    def in_hbm(*arrays):
        return [pltpu.with_memory_space_constraint(array, pltpu.HBM) for array in arrays]

    outgoing, slots = pl.pallas_call(
        pack_kernel,
        out_shape=(shape((sources, 1, 3 * points), f32), shape((columns * NB,), jnp.int32)),
        in_specs=[HBM] * 3,
        out_specs=(VMEM, SMEM),
        scratch_shapes=[
            pltpu.SMEM(table.shape, jnp.int32),
            pltpu.SMEM(counts.shape, jnp.int32),
            pltpu.VMEM((3, NB, points), f32),
            pltpu.SemaphoreType.DMA((3,)),
        ],
        compiler_params=params,
        name="pack",
    )(*in_hbm(table, counts, coords.transpose(1, 0, 2)))
    arrived = lax.all_to_all(outgoing, "grid", split_axis=0, concat_axis=0, tiled=True)
    spacing = exponents.reshape(-1, LANES)
    pieces, forward, backward, scale, work = pl.pallas_call(
        partial(prepare_kernel, group=sources // columns),
        out_shape=(
            shape((rows // BLK + cols // BLK, BLK, BLK), jnp.bfloat16),
            tile_shape,
            tile_shape,
            shape((3, NB * HALVES, LANES), f32),
            listed,
        ),
        in_specs=[HBM] * 7,
        out_specs=(VMEM,) * 4 + (SMEM,),
        scratch_shapes=[
            pltpu.SMEM(table.shape, jnp.int32),
            pltpu.SMEM(counts.shape, jnp.int32),
            pltpu.VMEM(centres.shape, f32),
            pltpu.VMEM(spacing.shape, f32),
            pltpu.VMEM(weights.shape, f32),
            pltpu.VMEM(core_density.shape, f32),
            pltpu.VMEM(density.shape, density.dtype),
            pltpu.VMEM((8 + BLK, LANES), f32),
            pltpu.SemaphoreType.DMA((7,)),
        ],
        compiler_params=params,
        name="prepare",
    )(*in_hbm(table, counts, centres, spacing, weights, core_density, density))
    most = 2 * (sources // GROUP)
    hold = pltpu.VMEM((2, GROUP, 2, BLK, LANES), f32)
    copy_sems = pltpu.SemaphoreType.DMA((2,))
    partials, done, kept = pl.pallas_call(
        density_kernel,
        out_shape=(
            messages,
            shape((most * GROUP + 8,), jnp.int32),
            pltpu.HBM((most, GROUP, 2, BLK, LANES), f32),
        ),
        in_specs=[SMEM] + [VMEM] * 4,
        out_specs=(VMEM, SMEM, HBM),
        scratch_shapes=[pltpu.SMEM((sources + 8,), jnp.int32), basis, hold, copy_sems],
        compiler_params=params,
        name="density",
    )(work, arrived, pieces, forward, backward)
    returned = lax.all_to_all(partials, "grid", split_axis=0, concat_axis=0, tiled=True)
    copies = pl.pallas_call(
        collect_kernel,
        out_shape=shape((columns, NB, 8, LANES), f32),
        in_specs=[SMEM, VMEM],
        out_specs=VMEM,
        compiler_params=params,
        name="collect",
    )(slots, returned)
    everything = lax.all_to_all(copies, "col", split_axis=0, concat_axis=0, tiled=True)
    sending, orbital_charge_samples, xc_batch_amounts = pl.pallas_call(
        point_kernel,
        out_shape=(messages, shape((NB, points), f32), shape((NB,), f32)),
        in_specs=[SMEM, VMEM, VMEM],
        out_specs=(VMEM, VMEM, SMEM),
        scratch_shapes=[
            pltpu.VMEM((NB * 8, LANES), f32),
            pltpu.VMEM((NB * 8, LANES), f32),
            pltpu.VMEM((2, NB * HALVES, LANES), f32),
        ],
        compiler_params=params,
        name="points",
    )(slots, everything, scale)
    factors = lax.all_to_all(sending, "grid", split_axis=0, concat_axis=0, tiled=True)
    potential_matrix_xc = pl.pallas_call(
        potential_kernel,
        out_shape=shape((rows, cols), f32),
        in_specs=[SMEM] + [VMEM] * 3 + [HBM],
        out_specs=VMEM,
        scratch_shapes=[basis, hold, copy_sems],
        compiler_params=params,
        name="potential",
    )(done, arrived, factors, pieces, *in_hbm(kept))
    return (potential_matrix_xc, orbital_charge_samples, xc_batch_amounts)


def solution(mesh):
    return jax.shard_map(
        local,
        mesh=mesh,
        in_specs=(
            P("grid", "col"),
            P(),
            P(),
            P("grid", None, None),
            P("grid", None),
            P("grid", None),
            P("grid"),
            P(),
        ),
        out_specs=(P("grid", "col"), P("grid", None), P("grid")),
        check_vma=False,
    )
```

```python
from functools import partial
import math

import jax
import jax.numpy as jnp
from jax import lax
from jax.experimental import pallas as pl
from jax.experimental.pallas import tpu as pltpu
from jax.sharding import PartitionSpec as P

BLK = 128
NB = 4
LANES = 128
HALVES = 2

kappa_pbe = 0.804
mu_coef = 0.2195
slater = -0.7385587663820224
grad_scale = 4.0 * (3.0 * math.pi**2) ** (2.0 / 3.0)
soft_square = 0.25

SMEM = pl.BlockSpec(memory_space=pltpu.SMEM)
VMEM = pl.BlockSpec(memory_space=pltpu.VMEM)


PIECES = 3
GROUP = 4
FAR = 64.0
LOG2E = math.log2(math.e)
SLOPE = 2.0 * math.log(2.0)
HBM = pl.BlockSpec(memory_space=pltpu.HBM)


def start_all(pairs, sems):
    copies = [
        pltpu.make_async_copy(source, target, sems.at[index])
        for index, (source, target) in enumerate(pairs)
    ]
    for copy in copies:
        copy.start()
    return copies


def pack_kernel(table_hbm, counts_hbm, coords_hbm, out, slots, table, counts, coords, sems):
    copies = start_all([(table_hbm, table), (counts_hbm, counts), (coords_hbm, coords)], sems)
    first = lax.axis_index("grid") * NB
    columns = table.shape[0]
    points = coords.shape[2]
    lane = lax.broadcasted_iota(jnp.int32, (1, points), 1)
    for copy in copies:
        copy.wait()
    for batch in range(NB):
        live = lane < counts[batch]
        message = jnp.concatenate(
            [jnp.where(live, coords[comp, pl.ds(batch, 1), :], FAR) for comp in range(3)], axis=1
        )
        for column in range(columns):
            slot = lax.shift_right_logical(table[column, first + batch], 1)
            slots[column * NB + batch] = slot
            out[slot] = message


def prepare_kernel(*refs, group):
    hbm, (pieces, forward, backward, scale, work) = refs[:7], refs[7:12]
    table, counts, centres, exponents, weights, core, density = refs[12:19]
    tile, sems = refs[19:]
    copies = start_all(list(zip(hbm, refs[12:19])), sems)
    rank = lax.axis_index("grid")
    column = lax.axis_index("col")
    own = rank // group
    row_blocks = density.shape[0] // BLK
    col_blocks = density.shape[1] // BLK
    sources = table.shape[1] // NB
    for copy in copies[:2]:
        copy.wait()

    def list_sources(step, filled):
        for unit in range(4):
            source = step * 4 + unit
            code = jnp.int32(0)
            for batch in range(NB):
                part = table[own, source * NB + batch] ^ (2 * rank)
                code = jnp.where(part < 2, 8 + 2 * batch + part, code)
            choice = lax.shift_right_logical(code, 1) & 3
            target = table[column, source * NB + choice] - column * col_blocks
            work[filled + 1] = source * 64 + (code & 1) * 32 + target * 2
            filled = filled + lax.shift_right_logical(code, 3)
        return filled

    filled = lax.fori_loop(0, sources // 4, list_sources, jnp.int32(0))
    close_list(work, filled)

    for copy in copies[4:6]:
        copy.wait()
    lane = lax.broadcasted_iota(jnp.int32, (1, LANES), 1)
    for batch in range(NB):
        for half in range(HALVES):
            place = pl.ds(batch * HALVES + half, 1)
            part = (pl.ds(batch, 1), pl.ds(half * LANES, LANES))
            live = jnp.where(lane + half * LANES < counts[batch], 1.0, 0.0).astype(jnp.float32)
            scale[0, place, :] = live
            scale[1, place, :] = weights[part] * live
            scale[2, place, :] = core[part]

    tile[...] = jnp.zeros_like(tile)

    def fill(block, slot):
        start = pl.multiple_of(block * BLK, BLK)
        tile[pl.ds(0, 3), :] = centres[:, pl.ds(start, BLK)]
        tile[pl.ds(3, 1), :] = exponents[pl.ds(block, 1), :] * (-LOG2E)
        rest = tile[pl.ds(0, 8), :]
        for index in range(PIECES):
            piece = rest.astype(jnp.bfloat16).astype(jnp.float32)
            tile[pl.ds((index + 1) * 8, 8), :] = piece
            rest = rest - piece
        pieces[slot] = tile[pl.ds(8, BLK), :].astype(jnp.bfloat16).T

    for copy in copies[2:4]:
        copy.wait()
    for slot in range(row_blocks):
        fill(rank * row_blocks + slot, slot)

    def fill_column(slot, carry):
        fill(column * col_blocks + slot, row_blocks + slot)
        start = pl.multiple_of(slot * BLK, BLK)
        for row in range(row_blocks):
            piece = density[pl.ds(row * BLK, BLK), pl.ds(start, BLK)]
            forward[slot, row] = piece
            backward[slot, row] = piece.T
        return carry

    copies[6].wait()
    lax.fori_loop(0, col_blocks, fill_column, 0)


def spread(pieces, basis):
    index = lax.broadcasted_iota(jnp.int32, (BLK, 4 * LANES), 0)
    lane = lax.broadcasted_iota(jnp.int32, (BLK, 4 * LANES), 1)
    picked = jnp.logical_and(index < 8 * PIECES, (index & 7) == lax.shift_right_logical(lane, 7))
    chooser = jnp.where(picked, 1.0, 0.0).astype(jnp.bfloat16)

    def fill(slot, carry):
        wide = jnp.dot(pieces[slot], chooser, preferred_element_type=jnp.float32)
        for comp in range(4):
            basis[slot, comp] = wide[:, comp * LANES : (comp + 1) * LANES]
        return carry

    lax.fori_loop(0, pieces.shape[0], fill, 0, unroll=2)


def side_of(basis, slot):
    return lambda comp: basis[slot, comp]


def total_rows(array):
    return jnp.sum(array, axis=0, keepdims=True)


def decode(entry):
    half = entry & 1
    block = lax.shift_right_logical(entry, 1) & 15
    row = lax.shift_right_logical(entry, 5) & 1
    source = lax.shift_right_logical(entry, 6)
    return source, row, block, half


def point_of(arrived, source, half):
    points = arrived.shape[2] // 3
    return [
        arrived[source, :, pl.ds(pl.multiple_of(comp * points + half * LANES, LANES), LANES)]
        for comp in range(3)
    ]


def values_of(side, point):
    offset = [point[comp] - side(comp) for comp in range(3)]
    distance = offset[0] * offset[0] + offset[1] * offset[1] + offset[2] * offset[2]
    return jnp.exp2(distance * side(3))


def close_list(work, filled):
    work[0] = filled
    for unit in range(1, GROUP):
        work[filled + unit] = work[jnp.maximum(filled, 1)]


def over_groups(work, handle, carry):
    filled = work[0]

    def group(step, carry):
        entries = [
            (work[GROUP * step + unit + 1], GROUP * step + unit < filled) for unit in range(GROUP)
        ]
        return handle(entries, carry)

    return lax.fori_loop(0, (filled + GROUP - 1) // GROUP, group, carry)


def over_halves(work, later, arrived, handle):
    def first_halves(entries, filled):
        for entry, real in entries:
            beyond = point_of(arrived, lax.shift_right_logical(entry, 6), 1)[0][0, 0]
            later[filled + 1] = entry + 1
            filled = filled + jnp.where(jnp.logical_and(beyond < FAR, real), 1, 0)
        handle(entries, 0)
        return filled

    close_list(later, over_groups(work, first_halves, jnp.int32(0)))
    over_groups(later, handle, 0)


def density_kernel(
    work, arrived, pieces, forward, backward, out, later, basis
):
    row_blocks = forward.shape[1]
    spread(pieces, basis)
    out[...] = jnp.zeros_like(out)

    def partial_sums(entry):
        source, row, block, half = decode(entry)
        point = point_of(arrived, source, half)
        row_side = side_of(basis, row)
        col_side = side_of(basis, row_blocks + block)

        row_values = values_of(row_side, point)
        col_values = values_of(col_side, point)
        right = jnp.dot(
            backward[block, row], row_values.astype(jnp.bfloat16), preferred_element_type=jnp.float32
        )
        left = jnp.dot(
            forward[block, row], col_values.astype(jnp.bfloat16), preferred_element_type=jnp.float32
        )
        col_product = col_values * right
        col_slope = col_product * col_side(3)
        row_slope = row_values * left * row_side(3)
        slope = total_rows(row_slope + col_slope)
        sums = [total_rows(col_product)]
        for comp in range(3):
            moment = total_rows(row_slope * row_side(comp) + col_slope * col_side(comp))
            sums.append(SLOPE * (point[comp] * slope - moment))
        return source, half, sums

    def halves(entries, carry):
        results = [partial_sums(entry) for entry, _ in entries]
        for source, half, sums in results:
            for comp in range(4):
                out[source, pl.ds(half * 4 + comp, 1), :] = sums[comp]
        return carry

    over_halves(work, later, arrived, halves)


def collect_kernel(slots, arrived, out):
    columns = slots.shape[0] // NB
    for batch in range(NB):
        total = arrived[slots[batch]]
        for column in range(1, columns):
            total = total + arrived[slots[column * NB + batch]]
        for copy in range(out.shape[0]):
            out[copy, batch] = total


def point_kernel(
    slots, sums, scale, out, charge_out, energy_out, summed, tiles, results_at
):
    columns = slots.shape[0] // NB
    for batch in range(NB):
        total = sums[0, batch]
        for column in range(1, sums.shape[0]):
            total = total + sums[column, batch]
        summed[pl.ds(batch * 8, 8), :] = total
    live = scale[0]
    point_scale = scale[1]
    count_rows = NB * HALVES
    valence = live * summed[pl.ds(0, count_rows, stride=4), :]
    gradient = [live * summed[pl.ds(comp + 1, count_rows, stride=4), :] for comp in range(3)]
    grad_square = (
        gradient[0] * gradient[0] + gradient[1] * gradient[1] + gradient[2] * gradient[2]
    )
    total = valence + scale[2]
    root = jnp.sqrt(total * total + soft_square)
    regular = 0.5 * (total + root)
    third = jnp.exp(jnp.log(regular) * (1.0 / 3.0))
    four_thirds = regular * third
    scaled = grad_scale * four_thirds * four_thirds
    weighted = mu_coef * grad_square
    inverse = 1.0 / (kappa_pbe * scaled + weighted)
    fraction = scaled * inverse
    enhance = 1.0 + kappa_pbe - kappa_pbe * kappa_pbe * fraction
    energy = slater * four_thirds * enhance
    square = kappa_pbe * kappa_pbe * mu_coef
    deriv_sigma = slater * four_thirds * (square * fraction * inverse)
    enhance_slope = (
        -(kappa_pbe * kappa_pbe)
        * (weighted * inverse)
        * inverse
        * (grad_scale * (8.0 / 3.0) * four_thirds * third)
    )
    deriv_regular = slater * ((4.0 / 3.0) * third * enhance + four_thirds * enhance_slope)
    deriv_density = deriv_regular * (0.5 * (1.0 + total / root))
    fweight = point_scale * deriv_density
    factor = 2.0 * point_scale * deriv_sigma
    results = [fweight] + [factor * gradient[comp] for comp in range(3)]
    for comp in range(4):
        tiles[pl.ds(comp, count_rows, stride=4), :] = results[comp]
    for batch in range(NB):
        tile = tiles[pl.ds(batch * 8, 8), :]
        for column in range(columns):
            out[slots[column * NB + batch]] = tile
    results_at[0] = valence
    results_at[1] = point_scale * energy
    for batch in range(NB):
        for half in range(HALVES):
            charge_out[pl.ds(batch, 1), pl.ds(half * LANES, LANES)] = results_at[
                0, pl.ds(batch * HALVES + half, 1), :
            ]
        energy_out[batch] = jnp.sum(results_at[1, pl.ds(batch * HALVES, HALVES), :])


def potential_kernel(work, arrived, factors, pieces, out, later, basis):
    row_blocks = out.shape[0] // BLK
    spread(pieces, basis)
    out[...] = jnp.zeros_like(out)

    def tile_of(entry, real):
        source, row, block, half = decode(entry)
        keep = jnp.where(real, 1.0, 0.0).astype(jnp.float32)
        point = point_of(arrived, source, half)
        factor = [factors[source, pl.ds(half * 4 + comp, 1), :] * keep for comp in range(4)]
        push = [SLOPE * factor[comp + 1] for comp in range(3)]
        along_point = push[0] * point[0] + push[1] * point[1] + push[2] * point[2]

        def turn(side):
            along_centre = push[0] * side(0) + push[1] * side(1) + push[2] * side(2)
            return (along_point - along_centre) * side(3)
        row_side = side_of(basis, row)
        col_side = side_of(basis, row_blocks + block)

        row_values = values_of(row_side, point)
        col_values = values_of(col_side, point)
        row_across = row_values * turn(row_side)
        along = col_values * (factor[0] + turn(col_side))
        left_side = jnp.concatenate(
            [row_values.astype(jnp.bfloat16), row_across.astype(jnp.bfloat16)], axis=1
        )
        right_side = jnp.concatenate(
            [along.astype(jnp.bfloat16), col_values.astype(jnp.bfloat16)], axis=1
        )
        product = lax.dot_general(
            left_side,
            right_side,
            (((1,), (1,)), ((), ())),
            preferred_element_type=jnp.float32,
        )
        row_start = pl.multiple_of(row * BLK, BLK)
        col_start = pl.multiple_of(block * BLK, BLK)
        return row_start, col_start, product

    def handle(entries, carry):
        results = [tile_of(entry, real) for entry, real in entries]
        for row_start, col_start, product in results:
            place = (pl.ds(row_start, BLK), pl.ds(col_start, BLK))
            out[place] = out[place] + product
        return carry

    over_halves(work, later, arrived, handle)


def local(density, centres, exponents, coords, weights, core_density, counts, blocks):
    sources = lax.axis_size("grid")
    columns = lax.axis_size("col")
    rows, cols = density.shape
    points = coords.shape[2]
    f32 = jnp.float32
    params = pltpu.CompilerParams(vmem_limit_bytes=16 * 1024 * 1024)
    table = blocks.T
    shape = jax.ShapeDtypeStruct
    messages = shape((sources, 8, LANES), f32)
    tile_shape = shape((cols // BLK, rows // BLK, BLK, BLK), jnp.bfloat16)
    basis = pltpu.VMEM((rows // BLK + cols // BLK, 4, BLK, LANES), f32)
    listed = shape((sources + 8,), jnp.int32)
    later = pltpu.SMEM(listed.shape, jnp.int32)

    def in_hbm(*arrays):
        return [pltpu.with_memory_space_constraint(array, pltpu.HBM) for array in arrays]

    outgoing, slots = pl.pallas_call(
        pack_kernel,
        out_shape=(shape((sources, 1, 3 * points), f32), shape((columns * NB,), jnp.int32)),
        in_specs=[HBM] * 3,
        out_specs=(VMEM, SMEM),
        scratch_shapes=[
            pltpu.SMEM(table.shape, jnp.int32),
            pltpu.SMEM(counts.shape, jnp.int32),
            pltpu.VMEM((3, NB, points), f32),
            pltpu.SemaphoreType.DMA((3,)),
        ],
        compiler_params=params,
        name="pack",
    )(*in_hbm(table, counts, coords.transpose(1, 0, 2)))
    arrived = lax.all_to_all(outgoing, "grid", split_axis=0, concat_axis=0, tiled=True)
    spacing = exponents.reshape(-1, LANES)
    pieces, forward, backward, scale, work = pl.pallas_call(
        partial(prepare_kernel, group=sources // columns),
        out_shape=(
            shape((rows // BLK + cols // BLK, BLK, BLK), jnp.bfloat16),
            tile_shape,
            tile_shape,
            shape((3, NB * HALVES, LANES), f32),
            listed,
        ),
        in_specs=[HBM] * 7,
        out_specs=(VMEM,) * 4 + (SMEM,),
        scratch_shapes=[
            pltpu.SMEM(table.shape, jnp.int32),
            pltpu.SMEM(counts.shape, jnp.int32),
            pltpu.VMEM(centres.shape, f32),
            pltpu.VMEM(spacing.shape, f32),
            pltpu.VMEM(weights.shape, f32),
            pltpu.VMEM(core_density.shape, f32),
            pltpu.VMEM(density.shape, density.dtype),
            pltpu.VMEM((8 + BLK, LANES), f32),
            pltpu.SemaphoreType.DMA((7,)),
        ],
        compiler_params=params,
        name="prepare",
    )(*in_hbm(table, counts, centres, spacing, weights, core_density, density))
    partials = pl.pallas_call(
        density_kernel,
        out_shape=messages,
        in_specs=[SMEM] + [VMEM] * 4,
        out_specs=VMEM,
        scratch_shapes=[later, basis],
        compiler_params=params,
        name="density",
    )(work, arrived, pieces, forward, backward)
    returned = lax.all_to_all(partials, "grid", split_axis=0, concat_axis=0, tiled=True)
    copies = pl.pallas_call(
        collect_kernel,
        out_shape=shape((columns, NB, 8, LANES), f32),
        in_specs=[SMEM, VMEM],
        out_specs=VMEM,
        compiler_params=params,
        name="collect",
    )(slots, returned)
    everything = lax.all_to_all(copies, "col", split_axis=0, concat_axis=0, tiled=True)
    sending, orbital_charge_samples, xc_batch_amounts = pl.pallas_call(
        point_kernel,
        out_shape=(messages, shape((NB, points), f32), shape((NB,), f32)),
        in_specs=[SMEM, VMEM, VMEM],
        out_specs=(VMEM, VMEM, SMEM),
        scratch_shapes=[
            pltpu.VMEM((NB * 8, LANES), f32),
            pltpu.VMEM((NB * 8, LANES), f32),
            pltpu.VMEM((2, NB * HALVES, LANES), f32),
        ],
        compiler_params=params,
        name="points",
    )(slots, everything, scale)
    factors = lax.all_to_all(sending, "grid", split_axis=0, concat_axis=0, tiled=True)
    potential_matrix_xc = pl.pallas_call(
        potential_kernel,
        out_shape=shape((rows, cols), f32),
        in_specs=[SMEM] + [VMEM] * 3,
        out_specs=VMEM,
        scratch_shapes=[later, basis],
        compiler_params=params,
        name="potential",
    )(work, arrived, factors, pieces)
    return (potential_matrix_xc, orbital_charge_samples, xc_batch_amounts)


def solution(mesh):
    return jax.shard_map(
        local,
        mesh=mesh,
        in_specs=(
            P("grid", "col"),
            P(),
            P(),
            P("grid", None, None),
            P("grid", None),
            P("grid", None),
            P("grid"),
            P(),
        ),
        out_specs=(P("grid", "col"), P("grid", None), P("grid")),
        check_vma=False,
    )
```

```python
from functools import partial
import math

import jax
import jax.numpy as jnp
from jax import lax
from jax.experimental import pallas as pl
from jax.experimental.pallas import tpu as pltpu
from jax.sharding import PartitionSpec as P

BLK = 128
NB = 4
LANES = 128
HALVES = 2

kappa_pbe = 0.804
mu_coef = 0.2195
slater = -0.7385587663820224
grad_scale = 4.0 * (3.0 * math.pi**2) ** (2.0 / 3.0)
soft_square = 0.25

SMEM = pl.BlockSpec(memory_space=pltpu.SMEM)
VMEM = pl.BlockSpec(memory_space=pltpu.VMEM)


PIECES = 3
GROUP = 4
FAR = 64.0
PARTS = 4
LOG2E = math.log2(math.e)
SLOPE = 2.0 * math.log(2.0)
HBM = pl.BlockSpec(memory_space=pltpu.HBM)


def start_all(pairs, sems):
    copies = [
        pltpu.make_async_copy(source, target, sems.at[index])
        for index, (source, target) in enumerate(pairs)
    ]
    for copy in copies:
        copy.start()
    return copies


def pack_kernel(table_hbm, counts_hbm, coords_hbm, out, slots, table, counts, coords, sems):
    copies = start_all([(table_hbm, table), (counts_hbm, counts), (coords_hbm, coords)], sems)
    first = lax.axis_index("grid") * NB
    columns = table.shape[0]
    points = coords.shape[2]
    lane = lax.broadcasted_iota(jnp.int32, (1, points), 1)
    for copy in copies:
        copy.wait()
    for batch in range(NB):
        live = lane < counts[batch]
        message = jnp.concatenate(
            [jnp.where(live, coords[comp, pl.ds(batch, 1), :], FAR) for comp in range(3)], axis=1
        )
        for column in range(columns):
            slot = lax.shift_right_logical(table[column, first + batch], 1)
            slots[column * NB + batch] = slot
            out[slot] = message


def prepare_kernel(*refs, group):
    hbm, (pieces, forward, backward, scale, work, upper, lower) = refs[:7], refs[7:14]
    table, counts, centres, exponents, weights, core, density = refs[14:21]
    tile, sems = refs[21:]
    copies = start_all(list(zip(hbm, refs[14:21])), sems)
    rank = lax.axis_index("grid")
    column = lax.axis_index("col")
    own = rank // group
    row_blocks = density.shape[0] // BLK
    col_blocks = density.shape[1] // BLK
    sources = table.shape[1] // NB
    for copy in copies[:2]:
        copy.wait()

    def list_sources(step, filled):
        every, high, low = filled
        for unit in range(4):
            source = step * 4 + unit
            code = jnp.int32(0)
            for batch in range(NB):
                part = table[own, source * NB + batch] ^ (2 * rank)
                code = jnp.where(part < 2, 8 + 2 * batch + part, code)
            choice = lax.shift_right_logical(code, 1) & 3
            target = table[column, source * NB + choice] - column * col_blocks
            entry = source * 64 + (code & 1) * 32 + target * 2
            work[every + 1] = entry
            upper[high + 1] = entry
            lower[low + 1] = entry
            found = lax.shift_right_logical(code, 3)
            every = every + found
            low = low + (found & code)
            high = every - low
        return every, high, low

    zero = jnp.int32(0)
    every, high, low = lax.fori_loop(0, sources // 4, list_sources, (zero, zero, zero))
    close_list(work, every)
    close_list(upper, high)
    close_list(lower, low)

    for copy in copies[4:6]:
        copy.wait()
    lane = lax.broadcasted_iota(jnp.int32, (1, LANES), 1)
    for batch in range(NB):
        for half in range(HALVES):
            place = pl.ds(batch * HALVES + half, 1)
            part = (pl.ds(batch, 1), pl.ds(half * LANES, LANES))
            live = jnp.where(lane + half * LANES < counts[batch], 1.0, 0.0).astype(jnp.float32)
            scale[0, place, :] = live
            scale[1, place, :] = weights[part] * live
            scale[2, place, :] = core[part]

    tile[...] = jnp.zeros_like(tile)

    def fill(block, slot):
        start = pl.multiple_of(block * BLK, BLK)
        tile[pl.ds(0, 3), :] = centres[:, pl.ds(start, BLK)]
        tile[pl.ds(3, 1), :] = exponents[pl.ds(block, 1), :] * (-LOG2E)
        rest = tile[pl.ds(0, 8), :]
        for index in range(PIECES):
            piece = rest.astype(jnp.bfloat16).astype(jnp.float32)
            tile[pl.ds((index + 1) * 8, 8), :] = piece
            rest = rest - piece
        pieces[slot] = tile[pl.ds(8, BLK), :].astype(jnp.bfloat16).T

    for copy in copies[2:4]:
        copy.wait()
    for slot in range(row_blocks):
        fill(rank * row_blocks + slot, slot)

    def fill_column(slot, carry):
        fill(column * col_blocks + slot, row_blocks + slot)
        start = pl.multiple_of(slot * BLK, BLK)
        for row in range(row_blocks):
            piece = density[pl.ds(row * BLK, BLK), pl.ds(start, BLK)]
            forward[slot, row] = piece
            backward[slot, row] = piece.T
        return carry

    copies[6].wait()
    lax.fori_loop(0, col_blocks, fill_column, 0)


def spread(pieces, basis):
    index = lax.broadcasted_iota(jnp.int32, (BLK, 4 * LANES), 0)
    lane = lax.broadcasted_iota(jnp.int32, (BLK, 4 * LANES), 1)
    picked = jnp.logical_and(index < 8 * PIECES, (index & 7) == lax.shift_right_logical(lane, 7))
    chooser = jnp.where(picked, 1.0, 0.0).astype(jnp.bfloat16)

    def fill(slot, carry):
        wide = jnp.dot(pieces[slot], chooser, preferred_element_type=jnp.float32)
        for comp in range(4):
            basis[slot, comp] = wide[:, comp * LANES : (comp + 1) * LANES]
        return carry

    lax.fori_loop(0, pieces.shape[0], fill, 0, unroll=2)


def side_of(basis, slot):
    return lambda comp: basis[slot, comp]


def total_rows(array):
    return jnp.sum(array, axis=0, keepdims=True)


def decode(entry):
    half = entry & 1
    block = lax.shift_right_logical(entry, 1) & 15
    row = lax.shift_right_logical(entry, 5) & 1
    source = lax.shift_right_logical(entry, 6)
    return source, row, block, half


def point_of(arrived, source, half):
    points = arrived.shape[2] // 3
    return [
        arrived[source, :, pl.ds(pl.multiple_of(comp * points + half * LANES, LANES), LANES)]
        for comp in range(3)
    ]


def values_of(side, point):
    offset = [point[comp] - side(comp) for comp in range(3)]
    distance = offset[0] * offset[0] + offset[1] * offset[1] + offset[2] * offset[2]
    return jnp.exp2(distance * side(3))


def close_list(work, filled):
    work[0] = filled
    for unit in range(1, GROUP):
        work[filled + unit] = work[jnp.maximum(filled, 1)]


def over_groups(work, handle, carry):
    filled = work[0]

    def group(step, carry):
        entries = [
            (work[GROUP * step + unit + 1], GROUP * step + unit < filled) for unit in range(GROUP)
        ]
        return handle(entries, carry)

    return lax.fori_loop(0, (filled + GROUP - 1) // GROUP, group, carry)


def over_halves(work, later, arrived, handle):
    def first_halves(entries, filled):
        for entry, real in entries:
            beyond = point_of(arrived, lax.shift_right_logical(entry, 6), 1)[0][0, 0]
            later[filled + 1] = entry + 1
            filled = filled + jnp.where(jnp.logical_and(beyond < FAR, real), 1, 0)
        handle(entries, 0)
        return filled

    close_list(later, over_groups(work, first_halves, jnp.int32(0)))
    over_groups(later, handle, 0)


def density_kernel(
    work, arrived, pieces, forward, backward, out, later, basis
):
    row_blocks = forward.shape[1]
    spread(pieces, basis)
    out[...] = jnp.zeros_like(out)

    def partial_sums(entry):
        source, row, block, half = decode(entry)
        point = point_of(arrived, source, half)
        row_side = side_of(basis, row)
        col_side = side_of(basis, row_blocks + block)

        row_values = values_of(row_side, point)
        col_values = values_of(col_side, point)
        right = jnp.dot(
            backward[block, row], row_values.astype(jnp.bfloat16), preferred_element_type=jnp.float32
        )
        left = jnp.dot(
            forward[block, row], col_values.astype(jnp.bfloat16), preferred_element_type=jnp.float32
        )
        col_product = col_values * right
        col_slope = col_product * col_side(3)
        row_slope = row_values * left * row_side(3)
        slope = total_rows(row_slope + col_slope)
        sums = [total_rows(col_product)]
        for comp in range(3):
            moment = total_rows(row_slope * row_side(comp) + col_slope * col_side(comp))
            sums.append(SLOPE * (point[comp] * slope - moment))
        return source, half, sums

    def halves(entries, carry):
        results = [partial_sums(entry) for entry, _ in entries]
        for source, half, sums in results:
            for comp in range(4):
                out[source, pl.ds(half * 4 + comp, 1), :] = sums[comp]
        return carry

    over_halves(work, later, arrived, halves)


def collect_kernel(slots, arrived, out):
    columns = slots.shape[0] // NB
    for batch in range(NB):
        total = arrived[slots[batch]]
        for column in range(1, columns):
            total = total + arrived[slots[column * NB + batch]]
        for copy in range(out.shape[0]):
            out[copy, batch] = total


def point_kernel(
    slots, sums, scale, out, charge_out, energy_out, summed, tiles, results_at
):
    columns = slots.shape[0] // NB
    for batch in range(NB):
        total = sums[0, batch]
        for column in range(1, sums.shape[0]):
            total = total + sums[column, batch]
        summed[pl.ds(batch * 8, 8), :] = total
    live = scale[0]
    point_scale = scale[1]
    count_rows = NB * HALVES
    valence = live * summed[pl.ds(0, count_rows, stride=4), :]
    gradient = [live * summed[pl.ds(comp + 1, count_rows, stride=4), :] for comp in range(3)]
    grad_square = (
        gradient[0] * gradient[0] + gradient[1] * gradient[1] + gradient[2] * gradient[2]
    )
    total = valence + scale[2]
    root = jnp.sqrt(total * total + soft_square)
    regular = 0.5 * (total + root)
    third = jnp.exp(jnp.log(regular) * (1.0 / 3.0))
    four_thirds = regular * third
    scaled = grad_scale * four_thirds * four_thirds
    weighted = mu_coef * grad_square
    inverse = 1.0 / (kappa_pbe * scaled + weighted)
    fraction = scaled * inverse
    enhance = 1.0 + kappa_pbe - kappa_pbe * kappa_pbe * fraction
    energy = slater * four_thirds * enhance
    square = kappa_pbe * kappa_pbe * mu_coef
    deriv_sigma = slater * four_thirds * (square * fraction * inverse)
    enhance_slope = (
        -(kappa_pbe * kappa_pbe)
        * (weighted * inverse)
        * inverse
        * (grad_scale * (8.0 / 3.0) * four_thirds * third)
    )
    deriv_regular = slater * ((4.0 / 3.0) * third * enhance + four_thirds * enhance_slope)
    deriv_density = deriv_regular * (0.5 * (1.0 + total / root))
    fweight = point_scale * deriv_density
    factor = 2.0 * point_scale * deriv_sigma
    results = [fweight] + [factor * gradient[comp] for comp in range(3)]
    for comp in range(4):
        tiles[pl.ds(comp, count_rows, stride=4), :] = results[comp]
    for batch in range(NB):
        tile = tiles[pl.ds(batch * 8, 8), :]
        for column in range(columns):
            out[slots[column * NB + batch]] = tile
    results_at[0] = valence
    results_at[1] = point_scale * energy
    for batch in range(NB):
        for half in range(HALVES):
            charge_out[pl.ds(batch, 1), pl.ds(half * LANES, LANES)] = results_at[
                0, pl.ds(batch * HALVES + half, 1), :
            ]
        energy_out[batch] = jnp.sum(results_at[1, pl.ds(batch * HALVES, HALVES), :])


def potential_kernel(upper, lower, arrived, factors, pieces, result, out, later, basis, sems):
    row_blocks = out.shape[0] // BLK
    spread(pieces, basis)
    out[...] = jnp.zeros_like(out)

    def tile_of(entry, real):
        source, row, block, half = decode(entry)
        keep = jnp.where(real, 1.0, 0.0).astype(jnp.float32)
        point = point_of(arrived, source, half)
        factor = [factors[source, pl.ds(half * 4 + comp, 1), :] * keep for comp in range(4)]
        push = [SLOPE * factor[comp + 1] for comp in range(3)]
        along_point = push[0] * point[0] + push[1] * point[1] + push[2] * point[2]

        def turn(side):
            along_centre = push[0] * side(0) + push[1] * side(1) + push[2] * side(2)
            return (along_point - along_centre) * side(3)
        row_side = side_of(basis, row)
        col_side = side_of(basis, row_blocks + block)

        row_values = values_of(row_side, point)
        col_values = values_of(col_side, point)
        row_across = row_values * turn(row_side)
        along = col_values * (factor[0] + turn(col_side))
        left_side = jnp.concatenate(
            [row_values.astype(jnp.bfloat16), row_across.astype(jnp.bfloat16)], axis=1
        )
        right_side = jnp.concatenate(
            [along.astype(jnp.bfloat16), col_values.astype(jnp.bfloat16)], axis=1
        )
        product = lax.dot_general(
            left_side,
            right_side,
            (((1,), (1,)), ((), ())),
            preferred_element_type=jnp.float32,
        )
        row_start = pl.multiple_of(row * BLK, BLK)
        col_start = pl.multiple_of(block * BLK, BLK)
        return row_start, col_start, product

    def handle(entries, carry):
        results = [tile_of(entry, real) for entry, real in entries]
        for row_start, col_start, product in results:
            place = (pl.ds(row_start, BLK), pl.ds(col_start, BLK))
            out[place] = out[place] + product
        return carry

    height = BLK // PARTS
    copies = []
    for row, work in enumerate((upper, lower)):
        over_halves(work, later, arrived, handle)
        for part in range(PARTS):
            place = (pl.ds(row * BLK + part * height, height), slice(None))
            copies.append(
                pltpu.make_async_copy(out.at[place], result.at[place], sems.at[row, part])
            )
            copies[-1].start()
    for copy in copies:
        copy.wait()


def local(density, centres, exponents, coords, weights, core_density, counts, blocks):
    sources = lax.axis_size("grid")
    columns = lax.axis_size("col")
    rows, cols = density.shape
    points = coords.shape[2]
    f32 = jnp.float32
    params = pltpu.CompilerParams(vmem_limit_bytes=16 * 1024 * 1024)
    table = blocks.T
    shape = jax.ShapeDtypeStruct
    messages = shape((sources, 8, LANES), f32)
    tile_shape = shape((cols // BLK, rows // BLK, BLK, BLK), jnp.bfloat16)
    basis = pltpu.VMEM((rows // BLK + cols // BLK, 4, BLK, LANES), f32)
    listed = shape((sources + 8,), jnp.int32)
    later = pltpu.SMEM(listed.shape, jnp.int32)

    def in_hbm(*arrays):
        return [pltpu.with_memory_space_constraint(array, pltpu.HBM) for array in arrays]

    outgoing, slots = pl.pallas_call(
        pack_kernel,
        out_shape=(shape((sources, 1, 3 * points), f32), shape((columns * NB,), jnp.int32)),
        in_specs=[HBM] * 3,
        out_specs=(VMEM, SMEM),
        scratch_shapes=[
            pltpu.SMEM(table.shape, jnp.int32),
            pltpu.SMEM(counts.shape, jnp.int32),
            pltpu.VMEM((3, NB, points), f32),
            pltpu.SemaphoreType.DMA((3,)),
        ],
        compiler_params=params,
        name="pack",
    )(*in_hbm(table, counts, coords.transpose(1, 0, 2)))
    arrived = lax.all_to_all(outgoing, "grid", split_axis=0, concat_axis=0, tiled=True)
    spacing = exponents.reshape(-1, LANES)
    pieces, forward, backward, scale, work, upper, lower = pl.pallas_call(
        partial(prepare_kernel, group=sources // columns),
        out_shape=(
            shape((rows // BLK + cols // BLK, BLK, BLK), jnp.bfloat16),
            tile_shape,
            tile_shape,
            shape((3, NB * HALVES, LANES), f32),
            listed,
            listed,
            listed,
        ),
        in_specs=[HBM] * 7,
        out_specs=(VMEM,) * 4 + (SMEM,) * 3,
        scratch_shapes=[
            pltpu.SMEM(table.shape, jnp.int32),
            pltpu.SMEM(counts.shape, jnp.int32),
            pltpu.VMEM(centres.shape, f32),
            pltpu.VMEM(spacing.shape, f32),
            pltpu.VMEM(weights.shape, f32),
            pltpu.VMEM(core_density.shape, f32),
            pltpu.VMEM(density.shape, density.dtype),
            pltpu.VMEM((8 + BLK, LANES), f32),
            pltpu.SemaphoreType.DMA((7,)),
        ],
        compiler_params=params,
        name="prepare",
    )(*in_hbm(table, counts, centres, spacing, weights, core_density, density))
    partials = pl.pallas_call(
        density_kernel,
        out_shape=messages,
        in_specs=[SMEM] + [VMEM] * 4,
        out_specs=VMEM,
        scratch_shapes=[later, basis],
        compiler_params=params,
        name="density",
    )(work, arrived, pieces, forward, backward)
    returned = lax.all_to_all(partials, "grid", split_axis=0, concat_axis=0, tiled=True)
    copies = pl.pallas_call(
        collect_kernel,
        out_shape=shape((columns, NB, 8, LANES), f32),
        in_specs=[SMEM, VMEM],
        out_specs=VMEM,
        compiler_params=params,
        name="collect",
    )(slots, returned)
    everything = lax.all_to_all(copies, "col", split_axis=0, concat_axis=0, tiled=True)
    sending, orbital_charge_samples, xc_batch_amounts = pl.pallas_call(
        point_kernel,
        out_shape=(messages, shape((NB, points), f32), shape((NB,), f32)),
        in_specs=[SMEM, VMEM, VMEM],
        out_specs=(VMEM, VMEM, SMEM),
        scratch_shapes=[
            pltpu.VMEM((NB * 8, LANES), f32),
            pltpu.VMEM((NB * 8, LANES), f32),
            pltpu.VMEM((2, NB * HALVES, LANES), f32),
        ],
        compiler_params=params,
        name="points",
    )(slots, everything, scale)
    factors = lax.all_to_all(sending, "grid", split_axis=0, concat_axis=0, tiled=True)
    potential_matrix_xc = pl.pallas_call(
        potential_kernel,
        out_shape=shape((rows, cols), f32),
        in_specs=[SMEM] * 2 + [VMEM] * 3,
        out_specs=HBM,
        scratch_shapes=[
            pltpu.VMEM((rows, cols), f32),
            later,
            basis,
            pltpu.SemaphoreType.DMA((2, PARTS)),
        ],
        compiler_params=params,
        name="potential",
    )(upper, lower, arrived, factors, pieces)
    return (potential_matrix_xc, orbital_charge_samples, xc_batch_amounts)


def solution(mesh):
    return jax.shard_map(
        local,
        mesh=mesh,
        in_specs=(
            P("grid", "col"),
            P(),
            P(),
            P("grid", None, None),
            P("grid", None),
            P("grid", None),
            P("grid"),
            P(),
        ),
        out_specs=(P("grid", "col"), P("grid", None), P("grid")),
        check_vma=False,
    )
```

```python
from functools import partial
import math

import jax
import jax.numpy as jnp
from jax import lax
from jax.experimental import pallas as pl
from jax.experimental.pallas import tpu as pltpu
from jax.sharding import PartitionSpec as P

BLK = 128
NB = 4
LANES = 128
HALVES = 2

kappa_pbe = 0.804
mu_coef = 0.2195
slater = -0.7385587663820224
grad_scale = 4.0 * (3.0 * math.pi**2) ** (2.0 / 3.0)
soft_square = 0.25

SMEM = pl.BlockSpec(memory_space=pltpu.SMEM)
VMEM = pl.BlockSpec(memory_space=pltpu.VMEM)


PIECES = 3
GROUP = 4
FAR = 64.0
LOG2E = math.log2(math.e)
SLOPE = 2.0 * math.log(2.0)
HBM = pl.BlockSpec(memory_space=pltpu.HBM)


def start_all(pairs, sems):
    copies = [
        pltpu.make_async_copy(source, target, sems.at[index])
        for index, (source, target) in enumerate(pairs)
    ]
    for copy in copies:
        copy.start()
    return copies


def pack_kernel(table_hbm, counts_hbm, coords_hbm, out, table, counts, coords, sems):
    copies = start_all([(table_hbm, table), (counts_hbm, counts), (coords_hbm, coords)], sems)
    first = lax.axis_index("grid") * NB
    columns = table.shape[0]
    points = coords.shape[2]
    lane = lax.broadcasted_iota(jnp.int32, (1, points), 1)
    for copy in copies:
        copy.wait()
    for batch in range(NB):
        live = lane < counts[batch]
        message = jnp.concatenate(
            [jnp.where(live, coords[comp, pl.ds(batch, 1), :], FAR) for comp in range(3)], axis=1
        )
        for column in range(columns):
            out[lax.shift_right_logical(table[column, first + batch], 1)] = message


def prepare_kernel(*refs, group):
    hbm, (pieces, forward, backward, scale, work, slots) = refs[:7], refs[7:13]
    table, counts, centres, exponents, weights, core, density = refs[13:20]
    tile, sems = refs[20:]
    copies = start_all(list(zip(hbm, refs[13:20])), sems)
    rank = lax.axis_index("grid")
    column = lax.axis_index("col")
    own = rank // group
    row_blocks = density.shape[0] // BLK
    col_blocks = density.shape[1] // BLK
    sources = table.shape[1] // NB
    for copy in copies[:2]:
        copy.wait()
    for batch in range(NB):
        for position in range(table.shape[0]):
            owner = lax.shift_right_logical(table[position, rank * NB + batch], 1)
            slots[position * NB + batch] = owner

    def list_sources(step, filled):
        for unit in range(4):
            source = step * 4 + unit
            code = jnp.int32(0)
            for batch in range(NB):
                part = table[own, source * NB + batch] ^ (2 * rank)
                code = jnp.where(part < 2, 8 + 2 * batch + part, code)
            choice = lax.shift_right_logical(code, 1) & 3
            target = table[column, source * NB + choice] - column * col_blocks
            work[filled + 1] = source * 64 + (code & 1) * 32 + target * 2
            filled = filled + lax.shift_right_logical(code, 3)
        return filled

    filled = lax.fori_loop(0, sources // 4, list_sources, jnp.int32(0))
    close_list(work, filled)

    for copy in copies[4:6]:
        copy.wait()
    lane = lax.broadcasted_iota(jnp.int32, (1, LANES), 1)
    for batch in range(NB):
        for half in range(HALVES):
            place = pl.ds(batch * HALVES + half, 1)
            part = (pl.ds(batch, 1), pl.ds(half * LANES, LANES))
            live = jnp.where(lane + half * LANES < counts[batch], 1.0, 0.0).astype(jnp.float32)
            scale[0, place, :] = live
            scale[1, place, :] = weights[part] * live
            scale[2, place, :] = core[part]

    tile[...] = jnp.zeros_like(tile)

    def fill(block, slot):
        start = pl.multiple_of(block * BLK, BLK)
        tile[pl.ds(0, 3), :] = centres[:, pl.ds(start, BLK)]
        tile[pl.ds(3, 1), :] = exponents[pl.ds(block, 1), :] * (-LOG2E)
        rest = tile[pl.ds(0, 8), :]
        for index in range(PIECES):
            piece = rest.astype(jnp.bfloat16).astype(jnp.float32)
            tile[pl.ds((index + 1) * 8, 8), :] = piece
            rest = rest - piece
        pieces[slot] = tile[pl.ds(8, BLK), :].astype(jnp.bfloat16).T

    for copy in copies[2:4]:
        copy.wait()
    for slot in range(row_blocks):
        fill(rank * row_blocks + slot, slot)

    def fill_column(slot, carry):
        fill(column * col_blocks + slot, row_blocks + slot)
        start = pl.multiple_of(slot * BLK, BLK)
        for row in range(row_blocks):
            piece = density[pl.ds(row * BLK, BLK), pl.ds(start, BLK)]
            forward[slot, row] = piece
            backward[slot, row] = piece.T
        return carry

    copies[6].wait()
    lax.fori_loop(0, col_blocks, fill_column, 0)


def spread(pieces, basis):
    index = lax.broadcasted_iota(jnp.int32, (BLK, 4 * LANES), 0)
    lane = lax.broadcasted_iota(jnp.int32, (BLK, 4 * LANES), 1)
    picked = jnp.logical_and(index < 8 * PIECES, (index & 7) == lax.shift_right_logical(lane, 7))
    chooser = jnp.where(picked, 1.0, 0.0).astype(jnp.bfloat16)

    def fill(slot, carry):
        wide = jnp.dot(pieces[slot], chooser, preferred_element_type=jnp.float32)
        for comp in range(4):
            basis[slot, comp] = wide[:, comp * LANES : (comp + 1) * LANES]
        return carry

    lax.fori_loop(0, pieces.shape[0], fill, 0, unroll=2)


def side_of(basis, slot):
    return lambda comp: basis[slot, comp]


def total_rows(array):
    return jnp.sum(array, axis=0, keepdims=True)


def decode(entry):
    half = entry & 1
    block = lax.shift_right_logical(entry, 1) & 15
    row = lax.shift_right_logical(entry, 5) & 1
    source = lax.shift_right_logical(entry, 6)
    return source, row, block, half


def point_of(arrived, source, half):
    points = arrived.shape[2] // 3
    return [
        arrived[source, :, pl.ds(pl.multiple_of(comp * points + half * LANES, LANES), LANES)]
        for comp in range(3)
    ]


def values_of(side, point):
    offset = [point[comp] - side(comp) for comp in range(3)]
    distance = offset[0] * offset[0] + offset[1] * offset[1] + offset[2] * offset[2]
    return jnp.exp2(distance * side(3))


def close_list(work, filled):
    work[0] = filled
    for unit in range(1, GROUP):
        work[filled + unit] = work[jnp.maximum(filled, 1)]


def over_groups(work, handle, carry):
    filled = work[0]

    def group(step, carry):
        entries = [
            (work[GROUP * step + unit + 1], GROUP * step + unit < filled) for unit in range(GROUP)
        ]
        return handle(entries, carry)

    return lax.fori_loop(0, (filled + GROUP - 1) // GROUP, group, carry)


def over_halves(work, later, arrived, handle):
    def first_halves(entries, filled):
        for entry, real in entries:
            beyond = point_of(arrived, lax.shift_right_logical(entry, 6), 1)[0][0, 0]
            later[filled + 1] = entry + 1
            filled = filled + jnp.where(jnp.logical_and(beyond < FAR, real), 1, 0)
        handle(entries, 0)
        return filled

    close_list(later, over_groups(work, first_halves, jnp.int32(0)))
    over_groups(later, handle, 0)


def density_kernel(
    work, arrived, pieces, forward, backward, out, later, basis
):
    row_blocks = forward.shape[1]
    spread(pieces, basis)
    out[...] = jnp.zeros_like(out)

    def partial_sums(entry):
        source, row, block, half = decode(entry)
        point = point_of(arrived, source, half)
        row_side = side_of(basis, row)
        col_side = side_of(basis, row_blocks + block)

        row_values = values_of(row_side, point)
        col_values = values_of(col_side, point)
        right = jnp.dot(
            backward[block, row], row_values.astype(jnp.bfloat16), preferred_element_type=jnp.float32
        )
        left = jnp.dot(
            forward[block, row], col_values.astype(jnp.bfloat16), preferred_element_type=jnp.float32
        )
        col_product = col_values * right
        col_slope = col_product * col_side(3)
        row_slope = row_values * left * row_side(3)
        slope = total_rows(row_slope + col_slope)
        sums = [total_rows(col_product)]
        for comp in range(3):
            moment = total_rows(row_slope * row_side(comp) + col_slope * col_side(comp))
            sums.append(SLOPE * (point[comp] * slope - moment))
        return source, half, sums

    def halves(entries, carry):
        results = [partial_sums(entry) for entry, _ in entries]
        for source, half, sums in results:
            for comp in range(4):
                out[source, pl.ds(half * 4 + comp, 1), :] = sums[comp]
        return carry

    over_halves(work, later, arrived, halves)


def collect_kernel(slots, arrived, out):
    columns = slots.shape[0] // NB
    for batch in range(NB):
        total = arrived[slots[batch]]
        for column in range(1, columns):
            total = total + arrived[slots[column * NB + batch]]
        for copy in range(out.shape[0]):
            out[copy, batch] = total


def point_kernel(
    slots, sums, scale, out, results_at, summed, tiles
):
    columns = slots.shape[0] // NB
    for batch in range(NB):
        total = sums[0, batch]
        for column in range(1, sums.shape[0]):
            total = total + sums[column, batch]
        summed[pl.ds(batch * 8, 8), :] = total
    live = scale[0]
    point_scale = scale[1]
    count_rows = NB * HALVES
    valence = live * summed[pl.ds(0, count_rows, stride=4), :]
    gradient = [live * summed[pl.ds(comp + 1, count_rows, stride=4), :] for comp in range(3)]
    grad_square = (
        gradient[0] * gradient[0] + gradient[1] * gradient[1] + gradient[2] * gradient[2]
    )
    total = valence + scale[2]
    root = jnp.sqrt(total * total + soft_square)
    regular = 0.5 * (total + root)
    third = jnp.exp(jnp.log(regular) * (1.0 / 3.0))
    four_thirds = regular * third
    scaled = grad_scale * four_thirds * four_thirds
    weighted = mu_coef * grad_square
    inverse = 1.0 / (kappa_pbe * scaled + weighted)
    fraction = scaled * inverse
    enhance = 1.0 + kappa_pbe - kappa_pbe * kappa_pbe * fraction
    energy = slater * four_thirds * enhance
    square = kappa_pbe * kappa_pbe * mu_coef
    deriv_sigma = slater * four_thirds * (square * fraction * inverse)
    enhance_slope = (
        -(kappa_pbe * kappa_pbe)
        * (weighted * inverse)
        * inverse
        * (grad_scale * (8.0 / 3.0) * four_thirds * third)
    )
    deriv_regular = slater * ((4.0 / 3.0) * third * enhance + four_thirds * enhance_slope)
    deriv_density = deriv_regular * (0.5 * (1.0 + total / root))
    fweight = point_scale * deriv_density
    factor = 2.0 * point_scale * deriv_sigma
    results = [fweight] + [factor * gradient[comp] for comp in range(3)]
    for comp in range(4):
        tiles[pl.ds(comp, count_rows, stride=4), :] = results[comp]
    for batch in range(NB):
        tile = tiles[pl.ds(batch * 8, 8), :]
        for column in range(columns):
            out[slots[column * NB + batch]] = tile
    results_at[0] = valence
    results_at[1] = point_scale * energy


def potential_kernel(
    work, arrived, factors, pieces, results_at, out, charge_out, energy_out, later, basis
):
    row_blocks = out.shape[0] // BLK
    spread(pieces, basis)
    out[...] = jnp.zeros_like(out)
    for batch in range(NB):
        for half in range(HALVES):
            charge_out[pl.ds(batch, 1), pl.ds(half * LANES, LANES)] = results_at[
                0, pl.ds(batch * HALVES + half, 1), :
            ]
        energy_out[batch] = jnp.sum(results_at[1, pl.ds(batch * HALVES, HALVES), :])

    def tile_of(entry, real):
        source, row, block, half = decode(entry)
        keep = jnp.where(real, 1.0, 0.0).astype(jnp.float32)
        point = point_of(arrived, source, half)
        factor = [factors[source, pl.ds(half * 4 + comp, 1), :] * keep for comp in range(4)]
        push = [SLOPE * factor[comp + 1] for comp in range(3)]
        along_point = push[0] * point[0] + push[1] * point[1] + push[2] * point[2]

        def turn(side):
            along_centre = push[0] * side(0) + push[1] * side(1) + push[2] * side(2)
            return (along_point - along_centre) * side(3)
        row_side = side_of(basis, row)
        col_side = side_of(basis, row_blocks + block)

        row_values = values_of(row_side, point)
        col_values = values_of(col_side, point)
        row_across = row_values * turn(row_side)
        along = col_values * (factor[0] + turn(col_side))
        left_side = jnp.concatenate(
            [row_values.astype(jnp.bfloat16), row_across.astype(jnp.bfloat16)], axis=1
        )
        right_side = jnp.concatenate(
            [along.astype(jnp.bfloat16), col_values.astype(jnp.bfloat16)], axis=1
        )
        product = lax.dot_general(
            left_side,
            right_side,
            (((1,), (1,)), ((), ())),
            preferred_element_type=jnp.float32,
        )
        row_start = pl.multiple_of(row * BLK, BLK)
        col_start = pl.multiple_of(block * BLK, BLK)
        return row_start, col_start, product

    def handle(entries, carry):
        results = [tile_of(entry, real) for entry, real in entries]
        for row_start, col_start, product in results:
            place = (pl.ds(row_start, BLK), pl.ds(col_start, BLK))
            out[place] = out[place] + product
        return carry

    over_halves(work, later, arrived, handle)


def local(density, centres, exponents, coords, weights, core_density, counts, blocks):
    sources = lax.axis_size("grid")
    columns = lax.axis_size("col")
    rows, cols = density.shape
    points = coords.shape[2]
    f32 = jnp.float32
    params = pltpu.CompilerParams(vmem_limit_bytes=16 * 1024 * 1024)
    table = blocks.T
    shape = jax.ShapeDtypeStruct
    messages = shape((sources, 8, LANES), f32)
    tile_shape = shape((cols // BLK, rows // BLK, BLK, BLK), jnp.bfloat16)
    basis = pltpu.VMEM((rows // BLK + cols // BLK, 4, BLK, LANES), f32)
    listed = shape((sources + 8,), jnp.int32)
    later = pltpu.SMEM(listed.shape, jnp.int32)

    def in_hbm(*arrays):
        return [pltpu.with_memory_space_constraint(array, pltpu.HBM) for array in arrays]

    outgoing = pl.pallas_call(
        pack_kernel,
        out_shape=shape((sources, 1, 3 * points), f32),
        in_specs=[HBM] * 3,
        out_specs=VMEM,
        scratch_shapes=[
            pltpu.SMEM(table.shape, jnp.int32),
            pltpu.SMEM(counts.shape, jnp.int32),
            pltpu.VMEM((3, NB, points), f32),
            pltpu.SemaphoreType.DMA((3,)),
        ],
        compiler_params=params,
        name="pack",
    )(*in_hbm(table, counts, coords.transpose(1, 0, 2)))
    arrived = lax.all_to_all(outgoing, "grid", split_axis=0, concat_axis=0, tiled=True)
    spacing = exponents.reshape(-1, LANES)
    pieces, forward, backward, scale, work, slots = pl.pallas_call(
        partial(prepare_kernel, group=sources // columns),
        out_shape=(
            shape((rows // BLK + cols // BLK, BLK, BLK), jnp.bfloat16),
            tile_shape,
            tile_shape,
            shape((3, NB * HALVES, LANES), f32),
            listed,
            shape((columns * NB,), jnp.int32),
        ),
        in_specs=[HBM] * 7,
        out_specs=(VMEM,) * 4 + (SMEM,) * 2,
        scratch_shapes=[
            pltpu.SMEM(table.shape, jnp.int32),
            pltpu.SMEM(counts.shape, jnp.int32),
            pltpu.VMEM(centres.shape, f32),
            pltpu.VMEM(spacing.shape, f32),
            pltpu.VMEM(weights.shape, f32),
            pltpu.VMEM(core_density.shape, f32),
            pltpu.VMEM(density.shape, density.dtype),
            pltpu.VMEM((8 + BLK, LANES), f32),
            pltpu.SemaphoreType.DMA((7,)),
        ],
        compiler_params=params,
        name="prepare",
    )(*in_hbm(table, counts, centres, spacing, weights, core_density, density))
    partials = pl.pallas_call(
        density_kernel,
        out_shape=messages,
        in_specs=[SMEM] + [VMEM] * 4,
        out_specs=VMEM,
        scratch_shapes=[later, basis],
        compiler_params=params,
        name="density",
    )(work, arrived, pieces, forward, backward)
    returned = lax.all_to_all(partials, "grid", split_axis=0, concat_axis=0, tiled=True)
    copies = pl.pallas_call(
        collect_kernel,
        out_shape=shape((columns, NB, 8, LANES), f32),
        in_specs=[SMEM, VMEM],
        out_specs=VMEM,
        compiler_params=params,
        name="collect",
    )(slots, returned)
    everything = lax.all_to_all(copies, "col", split_axis=0, concat_axis=0, tiled=True)
    sending, results = pl.pallas_call(
        point_kernel,
        out_shape=(messages, shape((2, NB * HALVES, LANES), f32)),
        in_specs=[SMEM, VMEM, VMEM],
        out_specs=(VMEM, VMEM),
        scratch_shapes=[pltpu.VMEM((NB * 8, LANES), f32), pltpu.VMEM((NB * 8, LANES), f32)],
        compiler_params=params,
        name="points",
    )(slots, everything, scale)
    factors = lax.all_to_all(sending, "grid", split_axis=0, concat_axis=0, tiled=True)
    potential_matrix_xc, orbital_charge_samples, xc_batch_amounts = pl.pallas_call(
        potential_kernel,
        out_shape=(shape((rows, cols), f32), shape((NB, points), f32), shape((NB,), f32)),
        in_specs=[SMEM] + [VMEM] * 4,
        out_specs=(VMEM, VMEM, SMEM),
        scratch_shapes=[later, basis],
        compiler_params=params,
        name="potential",
    )(work, arrived, factors, pieces, results)
    return (potential_matrix_xc, orbital_charge_samples, xc_batch_amounts)


def solution(mesh):
    return jax.shard_map(
        local,
        mesh=mesh,
        in_specs=(
            P("grid", "col"),
            P(),
            P(),
            P("grid", None, None),
            P("grid", None),
            P("grid", None),
            P("grid"),
            P(),
        ),
        out_specs=(P("grid", "col"), P("grid", None), P("grid")),
        check_vma=False,
    )
```
